32 devices in a mesh: dev: 32 (over z, y, x, core).
Axes of the slice: x: 2, y: 2, z: 4, core: 2. Of those that a mesh axis runs over, the one named last changes fastest.
Arguments:
- occurrence: bfloat16 [2048, 128, 128], P('dev'), may hold values from -0.5 to 0.5
- block_owner: int32 [2048, 1], P('dev'), may hold values from 0 to 31; in each aligned block of 64 rows (0 to 63, 64 to 127, ...) at most 4 rows name the same one
- read_block: int32 [2048], P('dev'), may hold values from 0 to 15
- slot_order: int32 [32, 128], P('dev'), may hold values from 0 to 127, each once within a row
Outputs:
- margin: float32 [65536, 512], P('dev')
The draws below stay inside these ranges and needn't reach their ends.
Inputs may be any that keep to these rules, and one draw needn't show every extreme that they name: `block_owner`: among the blocks of one device no owner is named more than 4 times, a bound that some block reaches. `slot_order`: each row names every number of 0 to 127 once.
All inputs are finite; a program needn't handle non-finite values.
Results may differ from the reference program's by a relative error of at most 0.0026.
Values may be sent and summed in bfloat16 or wider, within the bound.
A program may use at most 128 MiB of HBM per device.

```python
import math
import jax
import jax.numpy as jnp
import numpy as np
from jax import lax

RB = 128
KB = 128
CAP = 4
S_DEV = 64
RB_DEV = 16
PAIR_MOST = 4
BLOCKS = 2048
N_DEV = 32


def with_ends(array, stream_key, smallest, high):
    longest = array.shape.index(max(array.shape))
    spots = []
    for shift in (0, 1):
        where = [jax.random.randint(jax.random.fold_in(stream_key, axis), (), 0, length) for axis, length in enumerate(array.shape)]
        where[longest] = (where[longest] + shift) % array.shape[longest]
        spots.append(tuple(where))
    return array.at[spots[0]].set(smallest).at[spots[1]].set(high)


def level_of(own_key, dims, shards, smallest, high):
    gain, own = 1.0, jax.random.fold_in(own_key, 6)
    for axis_at, blocks in shards:
        heights = jnp.exp(jax.random.uniform(jax.random.fold_in(own, axis_at), (blocks,), jnp.float32, smallest / len(shards), high / len(shards)))
        gain = gain * jnp.repeat(heights, dims[axis_at] // blocks).reshape([-1 if axis == axis_at else 1 for axis in range(len(dims))])
    return gain


def shared_out(rng, own, number, rows, count, top, reach, lean):
    sequence = jax.random.permutation(rng, count)
    heavy_load, usual = shares(count, rows * top, reach, lean, True), shares(count, rows * top, reach, lean, False)
    places = jnp.arange(count)

    def named(sizes, turn):
        used = int((sizes > 0).sum())
        fixed = max(1, used // 4)
        moved = fixed + (places - fixed + turn * (used - fixed)) % max(1, count - fixed)
        return jnp.zeros((count,), jnp.int32).at[sequence[jnp.where(places < fixed, places, moved)]].set(jnp.asarray(sizes, jnp.int32))

    sizes = jnp.where(number % 4 == 0, named(heavy_load, number // 4), named(usual, number - number // 4 - 1))
    mixed = jax.random.permutation(jax.random.fold_in(own, 3), count)
    giver, taker = mixed[0:count // 2 * 2:2], mixed[1:count // 2 * 2:2]
    margin = jnp.minimum(sizes[giver] - 1, reach - sizes[taker]) // 2
    margin = jnp.where((giver == sequence[0]) | (taker == sequence[0]) | (sizes[taker] == 0), 0, jnp.maximum(margin, 0))
    moved = jax.random.randint(jax.random.fold_in(own, 4), (count // 2,), 0, 1 << 20) % (margin + 1)
    sizes = sizes.at[giver].add(-moved).at[taker].add(moved)
    labels = jnp.searchsorted(jnp.cumsum(sizes), jnp.arange(rows * top), side="right").astype(jnp.int32)
    table = labels.reshape(top, rows).T
    table = table[jax.random.permutation(jax.random.fold_in(own, 1), rows)]
    turn = jax.random.randint(jax.random.fold_in(own, 2), (rows, 1), 0, top)
    return jnp.take_along_axis(table, (jnp.arange(top)[None, :] + turn) % top, axis=1)


def shares(number_of, total, limit, lean, full):
    portions = [(1 << 20) // math.isqrt(grade ** lean) + 1 for grade in range(1, number_of + 1)]
    largest = limit if full else min(limit, max(-(-total // number_of), total * portions[0] // sum(portions)))
    least = 1 if total - largest >= number_of - 1 else 0
    counts, spare = [largest] + [least] * (number_of - 1), total - largest - least * (number_of - 1)
    while spare > 0:
        candidates = [i for i in range(1, number_of) if counts[i] < largest] or [i for i in range(1, number_of) if counts[i] < limit]
        whole, budget = sum([portions[i] for i in candidates]), spare
        for i in candidates:
            addition = min(limit - counts[i], max(1, budget * portions[i] // whole), spare)
            counts[i] = counts[i] + addition
            spare = spare - addition
    return np.array(counts)


def noise(key, extent, scale, reach, shards=(), held_as=jnp.bfloat16):
    loudness = level_of(key, extent, shards, -0.22, 0.18) if shards else 1.0
    drawn = jax.random.normal(key, extent, jnp.float32) * scale * loudness
    return jnp.minimum(jnp.maximum(drawn, -reach), reach).astype(held_as)


def setup_inputs(seed: int = 0) -> dict:
    arg_keys = jax.random.split(jax.random.key(seed), 5)
    occurrence = noise(arg_keys[0], (BLOCKS, RB, KB), KB ** -0.5, 0.5, ((0, 32),))
    block_owner_keys = jax.random.split(jax.random.fold_in(arg_keys[1], 1), BLOCKS // S_DEV)
    block_owner_turns = jax.random.permutation(jax.random.fold_in(arg_keys[1], 3), BLOCKS // S_DEV)
    block_owner = jax.vmap(lambda own, number: shared_out(jax.random.fold_in(arg_keys[1], 2), own, number, S_DEV, N_DEV, 1, PAIR_MOST, 2))(block_owner_keys, block_owner_turns).reshape((BLOCKS, 1))
    read_block = with_ends(jax.random.randint(arg_keys[2], (BLOCKS,), 0, RB_DEV), jax.random.fold_in(arg_keys[2], 1), 0, RB_DEV - 1).astype(jnp.int32)
    slot_order = jax.vmap(lambda own: jax.random.permutation(own, N_DEV * PAIR_MOST))(jax.random.split(arg_keys[3], N_DEV)).reshape((N_DEV, N_DEV * PAIR_MOST)).astype(jnp.int32)
    return dict(occurrence=occurrence, block_owner=block_owner, read_block=read_block, slot_order=slot_order)


def reference(occurrence, block_owner, read_block, slot_order):
    block_total = occurrence.shape[0]
    slot_total = N_DEV * PAIR_MOST
    owners = block_owner[:, 0].reshape(N_DEV, S_DEV)
    positions = jnp.arange(S_DEV, dtype=jnp.int32)
    earlier = positions[None, :] < positions[:, None]
    same_owner = owners[:, :, None] == owners[:, None, :]
    earlier_count = jnp.sum((same_owner & earlier[None]).astype(jnp.int32), axis=2).astype(jnp.int32)
    source = jnp.arange(N_DEV, dtype=jnp.int32)[:, None]
    slot_index = (source * PAIR_MOST + earlier_count).astype(jnp.int32)
    holder = jnp.full((N_DEV, slot_total), -1, jnp.int32)
    holder = holder.at[owners.reshape(-1), slot_index.reshape(-1)].set(jnp.arange(block_total, dtype=jnp.int32))
    ordered_holder = jnp.take_along_axis(holder, slot_order.astype(jnp.int32), axis=1)
    holder_safe = jnp.maximum(ordered_holder, 0)
    stacked = jnp.where((ordered_holder >= 0)[:, :, None, None], occurrence[holder_safe], jnp.zeros((), occurrence.dtype))
    groups = stacked.reshape(N_DEV, slot_total // CAP, CAP, RB, KB)
    owner_rows = jnp.arange(N_DEV, dtype=jnp.int32)[:, None] + jnp.zeros((1, slot_total), jnp.int32)
    place_of = jnp.zeros((N_DEV, slot_total), jnp.int32)
    place_of = place_of.at[owner_rows, slot_order.astype(jnp.int32)].set(
        jnp.zeros((N_DEV, 1), jnp.int32) + jnp.arange(slot_total, dtype=jnp.int32)[None, :])
    by_source = occurrence.reshape(N_DEV, S_DEV, RB, KB)
    read_rows = read_block.reshape(N_DEV, S_DEV)

    def one_source(carried, source_index):
        own_blocks = by_source[source_index]
        own_owner = owners[source_index]
        own_place = place_of[own_owner, slot_index[source_index]]
        group_blocks = groups[own_owner, own_place // CAP]
        tile_block = jnp.einsum('bik,bjrk->bijr', own_blocks.astype(jnp.float32), group_blocks.astype(jnp.float32))
        tile_block = tile_block.astype(jnp.bfloat16)
        onehot = (read_rows[source_index][None, :] == jnp.arange(RB_DEV, dtype=jnp.int32)[:, None]).astype(jnp.float32)
        summed = jnp.einsum('nb,bijr->nijr', onehot, tile_block.astype(jnp.float32))
        return carried, summed.reshape(RB_DEV * RB, CAP * RB)

    _, per_source = lax.scan(one_source, jnp.zeros((), jnp.float32), jnp.arange(N_DEV, dtype=jnp.int32))
    return per_source.reshape(N_DEV * RB_DEV * RB, CAP * RB)
```

```python
import functools
import jax
import jax.numpy as jnp
import numpy as np
from jax import lax
from jax.experimental import pallas as pl
from jax.experimental.pallas import tpu as pltpu
from jax.sharding import PartitionSpec as P

CAP = 4
RB_DEV = 16
CORES = 2
HALVES = 2
FAMILY = CORES * HALVES


def i32(x):
    return x.astype(jnp.int32)


def iota(*shape, axis):
    return lax.broadcasted_iota(jnp.int32, shape, axis)


def group_table(owners, order):
    devices, blocks = owners.shape
    slots = order.shape[1]
    per_pair = slots // devices
    earlier = iota(blocks, blocks, axis=1) < iota(blocks, blocks, axis=0)
    same = owners[:, :, None] == owners[:, None, :]
    rank = jnp.sum(i32(same & earlier[None]), axis=2)
    key = owners * per_pair + rank
    number = iota(devices, blocks, axis=0) * blocks + iota(devices, blocks, axis=1) + 1
    hit = key[:, :, None] == iota(1, 1, slots, axis=2)
    holder = jnp.sum(jnp.where(hit, number[:, :, None], 0), axis=1)
    holder = holder.reshape(devices, devices, per_pair).transpose(1, 0, 2).reshape(devices, slots)
    turned = order.reshape(devices, slots // CAP, CAP).transpose(2, 0, 1)
    hit = turned[:, :, :, None] == iota(1, 1, 1, slots, axis=3)
    table = jnp.sum(jnp.where(hit, holder[None, :, None, :], 0), axis=3)
    return table.reshape(CAP, devices * slots // CAP)


def fullest_lane(table, blocks):
    devices = lax.axis_size("dev")
    families = devices // FAMILY
    chips = devices // CORES
    source = jnp.where(table > 0, (table - 1) // blocks, -1)
    named = source[:, :, None] == iota(1, 1, devices, axis=2)
    held = jnp.sum(i32(named), axis=0)
    held_chip = jnp.sum(held.reshape(-1, chips, CORES), axis=2)
    demand = jnp.einsum(
        "gc,gd->cd",
        held_chip.astype(jnp.bfloat16),
        (held > 0).astype(jnp.bfloat16),
        preferred_element_type=jnp.float32,
    )
    c, d = iota(chips, devices, axis=0), iota(chips, devices, axis=1)
    return jnp.max(jnp.where(c % families != d // CORES % families, demand, 0.0))


def routes(table, blocks):
    devices = lax.axis_size("dev")
    families = devices // FAMILY
    half_devices = devices // HALVES
    many = FAMILY * blocks
    me = lax.axis_index("dev")
    half, family, core = me // half_devices, me // CORES % families, me % CORES
    x = jnp.arange(many, dtype=jnp.int32)
    x_half, x_core, x_block = x // (CORES * blocks), x // blocks % CORES, x % blocks
    ids = (((x_half * families + family) * CORES + x_core) * blocks + x_block + 1)[:, None]
    inside = (table[0][None] == ids) | (table[1][None] == ids)
    for j in range(2, CAP):
        inside = inside | (table[j][None] == ids)
    partners = jnp.stack(
        [jnp.sum(jnp.where(inside, table[j][None], 0), axis=1) for j in range(CAP)]
    )
    source = jnp.where(partners > 0, (partners - 1) // blocks, -1)
    target = iota(1, half_devices, axis=1) + half * half_devices
    named = source[:, :, None] == target[None]
    need = jnp.any(named, axis=0) & (target // CORES % families != family)
    row, column = iota(many, many, axis=0), iota(many, many, axis=1)
    same_chip = row // (CORES * blocks) == column // (CORES * blocks)
    before = ((column < row) & same_chip).astype(jnp.bfloat16)
    rank = i32(jnp.dot(before, need.astype(jnp.bfloat16), preferred_element_type=jnp.float32))
    rank = jnp.where(need, rank, -1).T
    local = (i32(x_half != half) * CORES + i32(x_core != core)) * blocks + x_block

    begin = half * CORES * blocks + core * blocks
    own = lax.dynamic_slice(partners, (0, begin), (CAP, blocks)).reshape(-1)
    total = devices * blocks
    match = own[:, None] == iota(1, total, axis=1) + 1
    wanted = jnp.any(match, axis=0).reshape(HALVES, families, CORES * blocks)
    wanted = wanted.transpose(1, 0, 2).reshape(families, many)
    arrived = i32(
        jnp.dot(wanted.astype(jnp.bfloat16), before.T, preferred_element_type=jnp.float32)
    )
    f = iota(families, many, axis=0)
    part = i32(iota(families, many, axis=1) // (CORES * blocks) != half)

    def send(begin, lane, far):
        spot = begin + iota(1, lane, 1, axis=1) * CORES + core
        chosen = jnp.where((x_half != half) == far, local % (CORES * blocks), 0)
        hit = (rank[:, None, :] == spot) & ((x_half != half) == far)
        return jnp.sum(jnp.where(hit, chosen[None, None, :], 0), axis=2).reshape(-1)

    def pick(begin, lane, local):
        empty = many + HALVES * half_devices * lane
        now = arrived - begin
        there = (part * half_devices + f * CORES + now % CORES) * lane + now // CORES + many
        there = jnp.where((now >= 0) & (now < lane * CORES), there, empty)
        place = jnp.where((f == family) & (begin == 0), local[None, :], jnp.where(f == family, empty, there))
        place = place.reshape(families, HALVES, CORES * blocks).transpose(1, 0, 2).reshape(1, total)
        found = jnp.sum(jnp.where(match, place, 0), axis=1)
        return jnp.where(own > 0, found, empty)

    return send, pick, local


def lane_sizes(blocks, devices):
    share = max(1, CORES * blocks * CORES // devices)
    early, late = CORES * ((5 * share + 3) // 4), CORES * ((7 * share + 3) // 4)
    kept = blocks // 4
    cross = 4 * (CORES * (blocks - kept) // 5)
    return early, late, kept, cross - cross % CORES


def chip_counts(table, blocks, kept):
    devices = lax.axis_size("dev")
    chips = devices // CORES
    source = jnp.where(table > 0, (table - 1) // (blocks * CORES), -1)
    spot = (table - 1) % blocks
    named = source[:, :, None] == iota(1, 1, chips, axis=2)
    held = jnp.sum(i32(named), axis=0)
    packed = jnp.sum(i32(named & (spot >= kept)[:, :, None]), axis=0)
    return held, packed


def too_full(table, blocks, early, late, kept, cross):
    devices = lax.axis_size("dev")
    chips = devices // CORES
    families = devices // FAMILY
    held, packed = chip_counts(table, blocks, kept)
    here = (held > 0).astype(jnp.bfloat16)
    demand = jnp.einsum(
        "gc,gd->cd", held.astype(jnp.bfloat16), here, preferred_element_type=jnp.float32
    )
    c, d = iota(chips, chips, axis=0), iota(chips, chips, axis=1)
    near = jnp.where(c // families == d // families, demand, 0.0)
    far = jnp.where(c // families != d // families, demand, 0.0)
    other = jnp.concatenate([far[families:], far[:families]], axis=0)
    load = other + jnp.maximum(near - early, 0.0)
    load = jnp.max(jnp.where(c % families != d % families, load, 0.0))
    halves = jnp.max(here.reshape(-1, HALVES, families), axis=2)
    crossing = jnp.einsum(
        "gc,gh->ch", packed.astype(jnp.bfloat16), halves, preferred_element_type=jnp.float32
    )
    c, h = iota(chips, HALVES, axis=0), iota(chips, HALVES, axis=1)
    crossing = jnp.max(jnp.where(c // families != h, crossing, 0.0))
    return (load > late) | (crossing > cross)


def plan(table, blocks, early, late, kept, cross):
    devices = lax.axis_size("dev")
    families = devices // FAMILY
    many = FAMILY * blocks
    pair = CORES * blocks
    me = lax.axis_index("dev")
    half, family, core = me // (devices // HALVES), me // CORES % families, me % CORES
    part = np.repeat(np.arange(HALVES), pair)
    x_core = np.tile(np.repeat(np.arange(CORES), blocks), HALVES)
    x_block = np.tile(np.arange(blocks), FAMILY)
    order = np.lexsort((x_block, x_core, (part == 1) & (x_block >= kept), part))
    part, x_core, x_block = (jnp.asarray(v[order], jnp.int32) for v in (part, x_core, x_block))
    x_half = jnp.where(half == 0, part, 1 - part)
    away = jnp.where(core == 0, x_core, 1 - x_core)

    ids = (((x_half * families + family) * CORES + x_core) * blocks + x_block + 1)[:, None]
    inside = (table[0][None] == ids) | (table[1][None] == ids)
    for j in range(2, CAP):
        inside = inside | (table[j][None] == ids)
    partners = jnp.stack(
        [jnp.sum(jnp.where(inside, table[j][None], 0), axis=1) for j in range(CAP)]
    )
    chip = jnp.where(partners > 0, (partners - 1) // pair, -1)
    f = iota(1, families, axis=1)
    need = jnp.any(chip[:, :, None] == (f + half * families)[None], axis=0) & (f != family)
    crosses = jnp.any((partners > 0) & (chip // families != x_half[None]), axis=0)
    crosses = crosses & (x_block >= kept)
    leaves, comes = crosses & (part == 0), crosses & (part == 1)
    wide = jnp.concatenate([need, leaves[:, None], comes[:, None]], axis=1)
    before = (iota(many, many, axis=1) < iota(many, many, axis=0)).astype(jnp.bfloat16)
    ranks = i32(jnp.dot(before, wide.astype(jnp.bfloat16), preferred_element_type=jnp.float32))
    ranks = jnp.where(wide, ranks, -1).T
    rank, leaving, coming = ranks[:families], ranks[families], ranks[families + 1]
    side = cross // CORES
    second = i32(coming >= side)
    packed = pair + CORES * kept
    packed = packed + jnp.where(core == 0, second, 1 - second) * side + coming - second * side
    local = jnp.where(
        part == 0,
        away * blocks + x_block,
        jnp.where(x_block < kept, pair + away * kept + x_block, packed),
    )

    spots = iota(1, side, 1, axis=1)[0] + core * side
    cross_send = jnp.sum(jnp.where(leaving[None] == spots, local[None], 0), axis=1)

    def send(first, stop, lane):
        spot = first[:, None, None] + iota(1, lane // CORES, 1, axis=1) + core * (lane // CORES)
        hit = (rank[:, None, :] == spot) & (rank[:, None, :] < stop[:, None, None])
        return jnp.sum(jnp.where(hit, local[None, None, :], 0), axis=2).reshape(-1)

    zero = jnp.zeros((families,), jnp.int32)
    near_count = jnp.sum(i32(need & (part == 0)[:, None]), axis=0)
    shipped = jnp.minimum(near_count, early)
    sends = send(zero, shipped, early), send(shipped, zero + many, late)

    pairs = partners[:, :pair].reshape(-1)
    all_ids = (
        ((x_half[None] * families + iota(families, 1, axis=0)) * CORES + x_core[None]) * blocks
        + x_block[None]
        + 1
    ).reshape(1, -1)
    wanted = jnp.any(pairs[:, None] == all_ids, axis=0).reshape(families, many)
    arrived = i32(
        jnp.dot(wanted.astype(jnp.bfloat16), before.T, preferred_element_type=jnp.float32)
    )
    came = jnp.sum(i32(wanted & (part == 0)[None]), axis=1, keepdims=True)
    came = jnp.minimum(came, early)
    base = pair + CORES * kept + cross
    g = iota(families, many, axis=0)
    place = jnp.where(
        arrived < came,
        base + g * early + arrived,
        base + families * early + g * late + arrived - came,
    )
    place = jnp.where(g == family, local[None], place).reshape(1, -1)
    empty = base + families * (early + late)
    own = lax.dynamic_slice(partners, (0, core * blocks), (CAP, blocks)).reshape(-1)
    found = jnp.sum(jnp.where(own[:, None] == all_ids, place, 0), axis=1)
    return cross_send, sends, jnp.where(own > 0, found, empty)


def fill(refs, held, sems):
    copies, at = [], 0
    for i, ref in enumerate(refs):
        copies.append(
            pltpu.make_async_copy(ref, held.at[pl.ds(at, ref.shape[0])], sems.at[i])
        )
        copies[-1].start()
        at += ref.shape[0]
    return copies


def pack_kernel(parts, *refs):
    sends, near = refs[:parts], refs[parts : -2 - parts]
    outs, (held, sems) = refs[-2 - parts : -2], refs[-2:]
    for copy in fill(near, held, sems):
        copy.wait()
    for send_ref, out_ref in zip(sends, outs):

        def step(i, _):
            out_ref[i] = held[send_ref[i]]
            return 0

        lax.fori_loop(0, out_ref.shape[0], step, 0, unroll=2)


def tile_kernel(pick_ref, read_ref, *refs):
    near, (out_ref, held, sems) = refs[:-3], refs[-3:]
    blocks, rows = near[0].shape[:2]
    copies = fill(near, held, sems)
    held[held.shape[0] - 1] = jnp.zeros(held.shape[1:], held.dtype)
    out_ref[...] = jnp.zeros_like(out_ref)
    for copy in copies:
        copy.wait()

    def step(b, _):
        others = jnp.concatenate([held[pick_ref[j * blocks + b]] for j in range(CAP)], axis=0)
        tile = lax.dot_general(
            held[b], others, (((1,), (1,)), ((), ())), preferred_element_type=jnp.float32
        )
        where = pl.ds(pl.multiple_of(read_ref[b] * rows, rows), rows)
        out_ref[where, :] += tile.astype(jnp.bfloat16).astype(jnp.float32)
        return 0

    lax.fori_loop(0, blocks, step, 0, unroll=2)


SMEM = pl.BlockSpec(memory_space=pltpu.SMEM)
HBM = pl.BlockSpec(memory_space=pl.ANY)
VMEM = pl.BlockSpec(memory_space=pltpu.VMEM)


def pack(sends, near):
    rows, kmers = near[0].shape[1:]
    total = sum(ref.shape[0] for ref in near)
    return pl.pallas_call(
        functools.partial(pack_kernel, len(sends)),
        out_shape=[
            jax.ShapeDtypeStruct((send.shape[0], rows, kmers), near[0].dtype) for send in sends
        ],
        in_specs=[SMEM] * len(sends) + [HBM] * len(near),
        out_specs=[VMEM] * len(sends),
        scratch_shapes=[
            pltpu.VMEM((total, rows, kmers), near[0].dtype),
            pltpu.SemaphoreType.DMA((len(near),)),
        ],
        compiler_params=pltpu.CompilerParams(vmem_limit_bytes=60 << 20),
        name="pack",
    )(*sends, *near)


def tiles(pick, read_block, near):
    rows, kmers = near[0].shape[1:]
    total = sum(ref.shape[0] for ref in near) + 1
    return pl.pallas_call(
        tile_kernel,
        out_shape=jax.ShapeDtypeStruct((RB_DEV * rows, CAP * rows), jnp.float32),
        in_specs=[SMEM, SMEM] + [HBM] * len(near),
        out_specs=VMEM,
        scratch_shapes=[
            pltpu.VMEM((total, rows, kmers), near[0].dtype),
            pltpu.SemaphoreType.DMA((len(near),)),
        ],
        compiler_params=pltpu.CompilerParams(vmem_limit_bytes=60 << 20),
        name="tiles",
    )(pick, read_block, *near)


def everyone_kernel(devices, group, row_ref, out_ref, send_sems, recv_sems):
    me = lax.axis_index("dev")
    first = me // group * group
    out_ref[me] = row_ref[...]

    def spread(src, dst, to, k):
        copy = pltpu.make_async_remote_copy(
            src_ref=src,
            dst_ref=dst,
            send_sem=send_sems.at[k],
            recv_sem=recv_sems.at[k],
            device_id=(to,),
            device_id_type=pl.DeviceIdType.MESH,
        )
        copy.start()
        return copy

    near = [
        spread(row_ref, out_ref.at[me], first + (me - first + k) % group, k)
        for k in range(1, group)
    ]
    for copy in near:
        copy.wait()
    rows = out_ref.at[pl.ds(first, group)]
    far = [
        spread(rows, rows, (me + k * group) % devices, group + k)
        for k in range(1, devices // group)
    ]
    for copy in far:
        copy.wait()


def gather_rows(row):
    devices = lax.axis_size("dev")
    group = 1 << devices.bit_length() // 2
    return pl.pallas_call(
        functools.partial(everyone_kernel, devices, group),
        out_shape=jax.ShapeDtypeStruct((devices,) + row.shape, row.dtype),
        in_specs=[VMEM],
        out_specs=VMEM,
        scratch_shapes=[pltpu.SemaphoreType.DMA((group + devices // group,))] * 2,
        compiler_params=pltpu.CompilerParams(has_side_effects=True),
        name="gather_rows",
    )(row)


def flipped(value, mask):
    bit = 1
    while bit <= mask:
        if mask & bit:
            value = value + bit - 2 * bit * (value // bit % 2)
        bit *= 2
    return value


def exchange_kernel(devices, lane, out_ref, got_ref, send_sems, recv_sems):
    me = lax.axis_index("dev")
    count = devices // HALVES
    spot = me % count

    def copy_of(k):
        to = flipped(spot, k)
        return pltpu.make_async_remote_copy(
            src_ref=out_ref.at[pl.ds(to * lane, lane)],
            dst_ref=got_ref.at[pl.ds(spot * lane, lane)],
            send_sem=send_sems.at[k],
            recv_sem=recv_sems.at[k],
            device_id=(me - spot + to,),
            device_id_type=pl.DeviceIdType.MESH,
        )

    chips = count // CORES
    steps = []
    for mask in range(chips - 1, chips // 2 - 1, -1):
        for core in range(CORES):
            masks = [m for m in (mask, chips - 1 - mask) if m]
            steps.append([copy_of(m * CORES + core) for m in masks])
    for i, step in enumerate(steps):
        if i >= 2:
            for copy in steps[i - 2]:
                copy.wait_send()
        for copy in step:
            copy.start()
    for step in steps[-2:]:
        for copy in step:
            copy.wait_send()
    for step in steps:
        for copy in step:
            copy.wait_recv()


def exchange(out, lane):
    devices = lax.axis_size("dev")
    count = devices // HALVES
    return pl.pallas_call(
        functools.partial(exchange_kernel, devices, lane),
        out_shape=jax.ShapeDtypeStruct(out.shape, out.dtype),
        in_specs=[HBM],
        out_specs=HBM,
        scratch_shapes=[pltpu.SemaphoreType.DMA((count,))] * 2,
        compiler_params=pltpu.CompilerParams(has_side_effects=True),
        cost_estimate=pl.CostEstimate(
            flops=0, bytes_accessed=32 * out.size * out.dtype.itemsize, transcendentals=0
        ),
        name="exchange",
    )(out)


def swap_kernel(families, lane, out_ref, got_ref, send_sems, recv_sems, pass_sems, take_sems):
    me = lax.axis_index("dev")
    chip, core = me // CORES, me % CORES
    spot = chip % families
    side = lane // CORES

    def copy_of(k):
        to = flipped(spot, k)
        return pltpu.make_async_remote_copy(
            src_ref=out_ref.at[pl.ds(to * side, side)],
            dst_ref=got_ref.at[pl.ds(spot * lane + core * side, side)],
            send_sem=send_sems.at[k],
            recv_sem=recv_sems.at[k],
            device_id=((chip - spot + to) * CORES + core,),
            device_id_type=pl.DeviceIdType.MESH,
        )

    def pass_of(k):
        rows = got_ref.at[pl.ds(flipped(spot, k) * lane + core * side, side)]
        return pltpu.make_async_remote_copy(
            src_ref=rows,
            dst_ref=rows,
            send_sem=pass_sems.at[k],
            recv_sem=take_sems.at[k],
            device_id=(chip * CORES + 1 - core,),
            device_id_type=pl.DeviceIdType.MESH,
        )

    masks = list(range(1, families))
    copies = {k: copy_of(k) for k in masks}
    passes = {k: pass_of(k) for k in masks}
    for k in reversed(masks):
        copies[k].start()
    for k in masks:
        copies[k].wait_recv()
        passes[k].start()
    for k in masks:
        passes[k].wait_recv()
    for k in masks:
        copies[k].wait_send()
        passes[k].wait_send()


def swap_lanes(out, lane):
    families = lax.axis_size("dev") // FAMILY
    return pl.pallas_call(
        functools.partial(swap_kernel, families, lane),
        out_shape=jax.ShapeDtypeStruct((families * lane,) + out.shape[1:], out.dtype),
        in_specs=[HBM],
        out_specs=HBM,
        scratch_shapes=[pltpu.SemaphoreType.DMA((families,))] * 4,
        compiler_params=pltpu.CompilerParams(has_side_effects=True),
        cost_estimate=pl.CostEstimate(
            flops=0, bytes_accessed=32 * out.size * out.dtype.itemsize, transcendentals=0
        ),
        name="swap_lanes",
    )(out)


def shards(occurrence, block_owner, read_block, slot_order):
    devices = lax.axis_size("dev")
    blocks = occurrence.shape[0]
    slots = slot_order.shape[1]
    spill = 2 * blocks // devices
    early, late, kept, cross = lane_sizes(blocks, devices)
    swap = [(d, d ^ 1) for d in range(devices)]
    across = [(d, (d + devices // HALVES) % devices) for d in range(devices)]
    row = jnp.stack([jnp.pad(block_owner[:, 0], (0, slots - blocks)), slot_order[0]])
    everyone = gather_rows(row)
    everyone, mine = lax.optimization_barrier((everyone, occurrence))
    far = lax.ppermute(mine[:kept], "dev", across)
    sibling = lax.ppermute(mine, "dev", swap)
    table = group_table(everyone[:, 0, :blocks], everyone[:, 1])
    cross_send, sends, pick = plan(table, blocks, early, late, kept, cross)
    full = too_full(table, blocks, early, late, kept, cross)
    crossing, out = pack((cross_send, sends[0]), (mine, sibling))
    crossed = lax.ppermute(crossing, "dev", across)
    got = swap_lanes(out, early)
    far, crossed, got = lax.optimization_barrier((far, crossed, got))
    near = (mine, sibling, far, lax.ppermute(far, "dev", swap))
    near = near + (crossed, lax.ppermute(crossed, "dev", swap))
    also = swap_lanes(pack((sends[1],), near)[0], late)
    first = tiles(pick, read_block, near + (got, also))

    def more(carry):
        begin, stop, margin = carry
        begin, now, mine = lax.optimization_barrier((begin, table, occurrence))
        send, pick, local = routes(now, blocks)
        sibling = lax.ppermute(mine, "dev", swap)
        far = lax.ppermute(mine, "dev", across)
        near = (mine, sibling, far, lax.ppermute(far, "dev", swap))
        got = exchange(pack((send(begin, spill, False),), near[:CORES])[0], spill)
        also = exchange(pack((send(begin, spill, True),), near[CORES:])[0], spill)
        added = tiles(pick(begin, spill, local), read_block, near + (got, also))
        margin = jnp.where(begin == 0, 0.0, margin) + added
        return begin + CORES * spill, i32(fullest_lane(now, blocks)), margin

    start = jnp.int32(0), jnp.where(full, 1, 0).astype(jnp.int32), first
    return lax.while_loop(lambda carry: carry[0] < carry[1], more, start)[2]


def solution(mesh):
    placed = (P("dev", None, None), P("dev", None), P("dev"), P("dev", None))
    return jax.shard_map(
        shards, mesh=mesh, in_specs=placed, out_specs=P("dev", None), check_vma=False
    )
```

```python
import functools
import jax
import jax.numpy as jnp
import numpy as np
from jax import lax
from jax.experimental import pallas as pl
from jax.experimental.pallas import tpu as pltpu
from jax.sharding import PartitionSpec as P

CAP = 4
RB_DEV = 16
CORES = 2
HALVES = 2
FAMILY = CORES * HALVES
AHEAD = 2
TOGETHER = 4


def i32(x):
    return x.astype(jnp.int32)


def iota(*shape, axis):
    return lax.broadcasted_iota(jnp.int32, shape, axis)


def group_table(owners, order):
    devices, blocks = owners.shape
    slots = order.shape[1]
    per_pair = slots // devices
    earlier = iota(blocks, blocks, axis=1) < iota(blocks, blocks, axis=0)
    same = owners[:, :, None] == owners[:, None, :]
    rank = jnp.sum(i32(same & earlier[None]), axis=2)
    key = owners * per_pair + rank
    number = iota(devices, blocks, axis=0) * blocks + iota(devices, blocks, axis=1) + 1
    hit = key[:, :, None] == iota(1, 1, slots, axis=2)
    holder = jnp.sum(jnp.where(hit, number[:, :, None], 0), axis=1)
    holder = holder.reshape(devices, devices, per_pair).transpose(1, 0, 2).reshape(devices, slots)
    turned = order.reshape(devices, slots // CAP, CAP).transpose(2, 0, 1)
    hit = turned[:, :, :, None] == iota(1, 1, 1, slots, axis=3)
    table = jnp.sum(jnp.where(hit, holder[None, :, None, :], 0), axis=3)
    return table.reshape(CAP, devices * slots // CAP)


def fullest_lane(table, blocks):
    devices = lax.axis_size("dev")
    families = devices // FAMILY
    chips = devices // CORES
    source = jnp.where(table > 0, (table - 1) // blocks, -1)
    named = source[:, :, None] == iota(1, 1, devices, axis=2)
    held = jnp.sum(i32(named), axis=0)
    held_chip = jnp.sum(held.reshape(-1, chips, CORES), axis=2)
    demand = jnp.einsum(
        "gc,gd->cd",
        held_chip.astype(jnp.bfloat16),
        (held > 0).astype(jnp.bfloat16),
        preferred_element_type=jnp.float32,
    )
    c, d = iota(chips, devices, axis=0), iota(chips, devices, axis=1)
    return jnp.max(jnp.where(c % families != d // CORES % families, demand, 0.0))


def routes(table, blocks):
    devices = lax.axis_size("dev")
    families = devices // FAMILY
    half_devices = devices // HALVES
    many = FAMILY * blocks
    me = lax.axis_index("dev")
    half, family, core = me // half_devices, me // CORES % families, me % CORES
    x = jnp.arange(many, dtype=jnp.int32)
    x_half, x_core, x_block = x // (CORES * blocks), x // blocks % CORES, x % blocks
    ids = (((x_half * families + family) * CORES + x_core) * blocks + x_block + 1)[:, None]
    inside = (table[0][None] == ids) | (table[1][None] == ids)
    for j in range(2, CAP):
        inside = inside | (table[j][None] == ids)
    partners = jnp.stack(
        [jnp.sum(jnp.where(inside, table[j][None], 0), axis=1) for j in range(CAP)]
    )
    source = jnp.where(partners > 0, (partners - 1) // blocks, -1)
    target = iota(1, half_devices, axis=1) + half * half_devices
    named = source[:, :, None] == target[None]
    need = jnp.any(named, axis=0) & (target // CORES % families != family)
    row, column = iota(many, many, axis=0), iota(many, many, axis=1)
    same_chip = row // (CORES * blocks) == column // (CORES * blocks)
    before = ((column < row) & same_chip).astype(jnp.bfloat16)
    rank = i32(jnp.dot(before, need.astype(jnp.bfloat16), preferred_element_type=jnp.float32))
    rank = jnp.where(need, rank, -1).T
    local = (i32(x_half != half) * CORES + i32(x_core != core)) * blocks + x_block

    begin = half * CORES * blocks + core * blocks
    own = lax.dynamic_slice(partners, (0, begin), (CAP, blocks)).reshape(-1)
    total = devices * blocks
    match = own[:, None] == iota(1, total, axis=1) + 1
    wanted = jnp.any(match, axis=0).reshape(HALVES, families, CORES * blocks)
    wanted = wanted.transpose(1, 0, 2).reshape(families, many)
    arrived = i32(
        jnp.dot(wanted.astype(jnp.bfloat16), before.T, preferred_element_type=jnp.float32)
    )
    f = iota(families, many, axis=0)
    part = i32(iota(families, many, axis=1) // (CORES * blocks) != half)

    def send(begin, lane, far):
        spot = begin + iota(1, lane, 1, axis=1) * CORES + core
        chosen = jnp.where((x_half != half) == far, local % (CORES * blocks), 0)
        hit = (rank[:, None, :] == spot) & ((x_half != half) == far)
        return jnp.sum(jnp.where(hit, chosen[None, None, :], 0), axis=2).reshape(-1)

    def pick(begin, lane, local):
        empty = many + HALVES * half_devices * lane
        now = arrived - begin
        there = (part * half_devices + f * CORES + now % CORES) * lane + now // CORES + many
        there = jnp.where((now >= 0) & (now < lane * CORES), there, empty)
        place = jnp.where((f == family) & (begin == 0), local[None, :], jnp.where(f == family, empty, there))
        place = place.reshape(families, HALVES, CORES * blocks).transpose(1, 0, 2).reshape(1, total)
        found = jnp.sum(jnp.where(match, place, 0), axis=1)
        return jnp.where(own > 0, found, empty)

    return send, pick, local


def lane_sizes(blocks, devices):
    share = max(1, CORES * blocks * CORES // devices)
    early, late = CORES * ((5 * share + 3) // 4), CORES * ((7 * share + 3) // 4)
    kept = blocks // 4
    cross = 4 * (CORES * (blocks - kept) // 5)
    return early, late, kept, cross - cross % CORES


def chip_counts(table, blocks, kept):
    devices = lax.axis_size("dev")
    chips = devices // CORES
    source = jnp.where(table > 0, (table - 1) // (blocks * CORES), -1)
    spot = (table - 1) % blocks
    named = source[:, :, None] == iota(1, 1, chips, axis=2)
    held = jnp.sum(i32(named), axis=0)
    packed = jnp.sum(i32(named & (spot >= kept)[:, :, None]), axis=0)
    return held, packed


def too_full(table, blocks, early, late, kept, cross):
    devices = lax.axis_size("dev")
    chips = devices // CORES
    families = devices // FAMILY
    held, packed = chip_counts(table, blocks, kept)
    here = (held > 0).astype(jnp.bfloat16)
    demand = jnp.einsum(
        "gc,gd->cd", held.astype(jnp.bfloat16), here, preferred_element_type=jnp.float32
    )
    c, d = iota(chips, chips, axis=0), iota(chips, chips, axis=1)
    near = jnp.where(c // families == d // families, demand, 0.0)
    far = jnp.where(c // families != d // families, demand, 0.0)
    other = jnp.concatenate([far[families:], far[:families]], axis=0)
    load = other + jnp.maximum(near - early, 0.0)
    load = jnp.max(jnp.where(c % families != d % families, load, 0.0))
    halves = jnp.max(here.reshape(-1, HALVES, families), axis=2)
    crossing = jnp.einsum(
        "gc,gh->ch", packed.astype(jnp.bfloat16), halves, preferred_element_type=jnp.float32
    )
    c, h = iota(chips, HALVES, axis=0), iota(chips, HALVES, axis=1)
    crossing = jnp.max(jnp.where(c // families != h, crossing, 0.0))
    return (load > late) | (crossing > cross)


def plan(table, blocks, early, late, kept, cross):
    devices = lax.axis_size("dev")
    families = devices // FAMILY
    many = FAMILY * blocks
    pair = CORES * blocks
    me = lax.axis_index("dev")
    half, family, core = me // (devices // HALVES), me // CORES % families, me % CORES
    part = np.repeat(np.arange(HALVES), pair)
    x_core = np.tile(np.repeat(np.arange(CORES), blocks), HALVES)
    x_block = np.tile(np.arange(blocks), FAMILY)
    order = np.lexsort((x_block, x_core, (part == 1) & (x_block >= kept), part))
    part, x_core, x_block = (jnp.asarray(v[order], jnp.int32) for v in (part, x_core, x_block))
    x_half = jnp.where(half == 0, part, 1 - part)
    away = jnp.where(core == 0, x_core, 1 - x_core)

    ids = (((x_half * families + family) * CORES + x_core) * blocks + x_block + 1)[:, None]
    inside = (table[0][None] == ids) | (table[1][None] == ids)
    for j in range(2, CAP):
        inside = inside | (table[j][None] == ids)
    partners = jnp.stack(
        [jnp.sum(jnp.where(inside, table[j][None], 0), axis=1) for j in range(CAP)]
    )
    chip = jnp.where(partners > 0, (partners - 1) // pair, -1)
    f = iota(1, families, axis=1)
    need = jnp.any(chip[:, :, None] == (f + half * families)[None], axis=0) & (f != family)
    crosses = jnp.any((partners > 0) & (chip // families != x_half[None]), axis=0)
    crosses = crosses & (x_block >= kept)
    leaves, comes = crosses & (part == 0), crosses & (part == 1)
    wide = jnp.concatenate([need, leaves[:, None], comes[:, None]], axis=1)
    before = (iota(many, many, axis=1) < iota(many, many, axis=0)).astype(jnp.bfloat16)
    ranks = i32(jnp.dot(before, wide.astype(jnp.bfloat16), preferred_element_type=jnp.float32))
    ranks = jnp.where(wide, ranks, -1).T
    rank, leaving, coming = ranks[:families], ranks[families], ranks[families + 1]
    side = cross // CORES
    second = i32(coming >= side)
    packed = pair + CORES * kept
    packed = packed + jnp.where(core == 0, second, 1 - second) * side + coming - second * side
    local = jnp.where(
        part == 0,
        away * blocks + x_block,
        jnp.where(x_block < kept, pair + away * kept + x_block, packed),
    )

    spots = iota(1, side, 1, axis=1)[0] + core * side
    cross_send = jnp.sum(jnp.where(leaving[None] == spots, local[None], 0), axis=1)

    def send(first, stop, lane):
        spot = first[:, None, None] + iota(1, lane // CORES, 1, axis=1) + core * (lane // CORES)
        hit = (rank[:, None, :] == spot) & (rank[:, None, :] < stop[:, None, None])
        return jnp.sum(jnp.where(hit, local[None, None, :], 0), axis=2).reshape(-1)

    zero = jnp.zeros((families,), jnp.int32)
    near_count = jnp.sum(i32(need & (part == 0)[:, None]), axis=0)
    shipped = jnp.minimum(near_count, early)
    sends = send(zero, shipped, early), send(shipped, zero + many, late)

    pairs = partners[:, :pair].reshape(-1)
    all_ids = (
        ((x_half[None] * families + iota(families, 1, axis=0)) * CORES + x_core[None]) * blocks
        + x_block[None]
        + 1
    ).reshape(1, -1)
    wanted = jnp.any(pairs[:, None] == all_ids, axis=0).reshape(families, many)
    arrived = i32(
        jnp.dot(wanted.astype(jnp.bfloat16), before.T, preferred_element_type=jnp.float32)
    )
    came = jnp.sum(i32(wanted & (part == 0)[None]), axis=1, keepdims=True)
    came = jnp.minimum(came, early)
    base = pair + CORES * kept + cross
    g = iota(families, many, axis=0)
    place = jnp.where(
        arrived < came,
        base + g * early + arrived,
        base + families * early + g * late + arrived - came,
    )
    place = jnp.where(g == family, local[None], place).reshape(1, -1)
    empty = base + families * (early + late)
    own = lax.dynamic_slice(partners, (0, core * blocks), (CAP, blocks)).reshape(-1)
    found = jnp.sum(jnp.where(own[:, None] == all_ids, place, 0), axis=1)
    return cross_send, sends, jnp.where(own > 0, found, empty)


def fill(refs, held, sems):
    copies, at = [], 0
    for i, ref in enumerate(refs):
        copies.append(
            pltpu.make_async_copy(ref, held.at[pl.ds(at, ref.shape[0])], sems.at[i])
        )
        copies[-1].start()
        at += ref.shape[0]
    return copies


def pack_kernel(parts, *refs):
    sends, near = refs[:parts], refs[parts : -2 - parts]
    outs, (held, sems) = refs[-2 - parts : -2], refs[-2:]
    for copy in fill(near, held, sems):
        copy.wait()
    for send_ref, out_ref in zip(sends, outs):

        def step(i, _):
            out_ref[i] = held[send_ref[i]]
            return 0

        lax.fori_loop(0, out_ref.shape[0], step, 0, unroll=2)


def tile_kernel(pick_ref, read_ref, *refs):
    near, (out_ref, held, sems) = refs[:-3], refs[-3:]
    blocks, rows = near[0].shape[:2]
    copies = fill(near, held, sems)
    held[held.shape[0] - 1] = jnp.zeros(held.shape[1:], held.dtype)
    out_ref[...] = jnp.zeros_like(out_ref)
    for copy in copies:
        copy.wait()

    def tile_of(b):
        others = jnp.concatenate([held[pick_ref[j * blocks + b]] for j in range(CAP)], axis=0)
        tile = lax.dot_general(
            held[b], others, (((1,), (1,)), ((), ())), preferred_element_type=jnp.float32
        )
        return tile.astype(jnp.bfloat16)

    def step(i, _):
        found = [tile_of(i * TOGETHER + k) for k in range(TOGETHER)]
        for k in range(TOGETHER):
            begin = read_ref[i * TOGETHER + k] * rows
            where = pl.ds(pl.multiple_of(begin, rows), rows)
            out_ref[where, :] += found[k].astype(jnp.float32)
        return 0

    lax.fori_loop(0, blocks // TOGETHER, step, 0, unroll=2)


SMEM = pl.BlockSpec(memory_space=pltpu.SMEM)
HBM = pl.BlockSpec(memory_space=pl.ANY)
VMEM = pl.BlockSpec(memory_space=pltpu.VMEM)


def pack(sends, near):
    rows, kmers = near[0].shape[1:]
    total = sum(ref.shape[0] for ref in near)
    return pl.pallas_call(
        functools.partial(pack_kernel, len(sends)),
        out_shape=[
            jax.ShapeDtypeStruct((send.shape[0], rows, kmers), near[0].dtype) for send in sends
        ],
        in_specs=[SMEM] * len(sends) + [HBM] * len(near),
        out_specs=[VMEM] * len(sends),
        scratch_shapes=[
            pltpu.VMEM((total, rows, kmers), near[0].dtype),
            pltpu.SemaphoreType.DMA((len(near),)),
        ],
        compiler_params=pltpu.CompilerParams(vmem_limit_bytes=60 << 20),
        name="pack",
    )(*sends, *near)


def tiles(pick, read_block, near):
    rows, kmers = near[0].shape[1:]
    total = sum(ref.shape[0] for ref in near) + 1
    return pl.pallas_call(
        tile_kernel,
        out_shape=jax.ShapeDtypeStruct((RB_DEV * rows, CAP * rows), jnp.float32),
        in_specs=[SMEM, SMEM] + [HBM] * len(near),
        out_specs=VMEM,
        scratch_shapes=[
            pltpu.VMEM((total, rows, kmers), near[0].dtype),
            pltpu.SemaphoreType.DMA((len(near),)),
        ],
        compiler_params=pltpu.CompilerParams(vmem_limit_bytes=60 << 20),
        name="tiles",
    )(pick, read_block, *near)


def greet(others):
    barrier = pltpu.get_barrier_semaphore()
    for other in others:
        pl.semaphore_signal(
            barrier, inc=1, device_id=(other,), device_id_type=pl.DeviceIdType.MESH
        )
    pl.semaphore_wait(barrier, len(others))


def everyone_kernel(devices, row_ref, out_ref, send_sems, recv_sems):
    me = lax.axis_index("dev")
    out_ref[me] = row_ref[...]
    greet([(me + k) % devices for k in range(1, devices)])
    copies = [
        pltpu.make_async_remote_copy(
            src_ref=row_ref,
            dst_ref=out_ref.at[me],
            send_sem=send_sems.at[k],
            recv_sem=recv_sems.at[k],
            device_id=((me + k) % devices,),
            device_id_type=pl.DeviceIdType.MESH,
        )
        for k in range(1, devices)
    ]
    for copy in copies:
        copy.start()
    for copy in copies:
        copy.wait()


def gather_rows(row):
    devices = lax.axis_size("dev")
    return pl.pallas_call(
        functools.partial(everyone_kernel, devices),
        out_shape=jax.ShapeDtypeStruct((devices,) + row.shape, row.dtype),
        in_specs=[VMEM],
        out_specs=VMEM,
        scratch_shapes=[pltpu.SemaphoreType.DMA((devices,))] * 2,
        compiler_params=pltpu.CompilerParams(has_side_effects=True, collective_id=0),
        name="gather_rows",
    )(row)


def flipped(value, mask):
    bit = 1
    while bit <= mask:
        if mask & bit:
            value = value + bit - 2 * bit * (value // bit % 2)
        bit *= 2
    return value


def exchange_kernel(devices, lane, out_ref, got_ref, send_sems, recv_sems):
    me = lax.axis_index("dev")
    count = devices // HALVES
    spot = me % count

    def copy_of(k):
        to = flipped(spot, k)
        return pltpu.make_async_remote_copy(
            src_ref=out_ref.at[pl.ds(to * lane, lane)],
            dst_ref=got_ref.at[pl.ds(spot * lane, lane)],
            send_sem=send_sems.at[k],
            recv_sem=recv_sems.at[k],
            device_id=(me - spot + to,),
            device_id_type=pl.DeviceIdType.MESH,
        )

    chips = count // CORES
    steps = []
    for mask in range(chips - 1, chips // 2 - 1, -1):
        for core in range(CORES):
            masks = [m for m in (mask, chips - 1 - mask) if m]
            steps.append([copy_of(m * CORES + core) for m in masks])
    for i, step in enumerate(steps):
        if i >= 2:
            for copy in steps[i - 2]:
                copy.wait_send()
        for copy in step:
            copy.start()
    for step in steps[-2:]:
        for copy in step:
            copy.wait_send()
    for step in steps:
        for copy in step:
            copy.wait_recv()


def exchange(out, lane):
    devices = lax.axis_size("dev")
    count = devices // HALVES
    return pl.pallas_call(
        functools.partial(exchange_kernel, devices, lane),
        out_shape=jax.ShapeDtypeStruct(out.shape, out.dtype),
        in_specs=[HBM],
        out_specs=HBM,
        scratch_shapes=[pltpu.SemaphoreType.DMA((count,))] * 2,
        compiler_params=pltpu.CompilerParams(has_side_effects=True),
        cost_estimate=pl.CostEstimate(
            flops=0, bytes_accessed=32 * out.size * out.dtype.itemsize, transcendentals=0
        ),
        name="exchange",
    )(out)


def swap_kernel(families, lane, out_ref, got_ref, send_sems, recv_sems, pass_sems, take_sems):
    me = lax.axis_index("dev")
    chip, core = me // CORES, me % CORES
    spot = chip % families
    side = lane // CORES

    def copy_of(k):
        to = flipped(spot, k)
        return pltpu.make_async_remote_copy(
            src_ref=out_ref.at[pl.ds(to * side, side)],
            dst_ref=got_ref.at[pl.ds(spot * lane + core * side, side)],
            send_sem=send_sems.at[k],
            recv_sem=recv_sems.at[k],
            device_id=((chip - spot + to) * CORES + core,),
            device_id_type=pl.DeviceIdType.MESH,
        )

    def pass_of(k):
        rows = got_ref.at[pl.ds(flipped(spot, k) * lane + core * side, side)]
        return pltpu.make_async_remote_copy(
            src_ref=rows,
            dst_ref=rows,
            send_sem=pass_sems.at[k],
            recv_sem=take_sems.at[k],
            device_id=(chip * CORES + 1 - core,),
            device_id_type=pl.DeviceIdType.MESH,
        )

    chips = [(chip - spot + flipped(spot, k)) * CORES + core for k in range(1, families)]
    greet(chips + [chip * CORES + 1 - core])
    top = families - 1
    steps = [[k for k in (m, top - m) if k] for m in range(top, families // 2 - 1, -1)]
    copies = [[copy_of(k) for k in step] for step in steps]
    passes = [[pass_of(k) for k in step] for step in steps]
    for i in range(len(steps) + AHEAD):
        if i >= AHEAD:
            for copy in copies[i - AHEAD]:
                copy.wait_send()
        if i < len(steps):
            for copy in copies[i]:
                copy.start()
        if i >= AHEAD:
            for copy, follow in zip(copies[i - AHEAD], passes[i - AHEAD]):
                copy.wait_recv()
                follow.start()
    for step in passes:
        for follow in step:
            follow.wait()


def swap_lanes(out, lane, number):
    families = lax.axis_size("dev") // FAMILY
    return pl.pallas_call(
        functools.partial(swap_kernel, families, lane),
        out_shape=jax.ShapeDtypeStruct((families * lane,) + out.shape[1:], out.dtype),
        in_specs=[HBM],
        out_specs=HBM,
        scratch_shapes=[pltpu.SemaphoreType.DMA((families,))] * 4,
        compiler_params=pltpu.CompilerParams(has_side_effects=True, collective_id=number),
        cost_estimate=pl.CostEstimate(
            flops=0, bytes_accessed=32 * out.size * out.dtype.itemsize, transcendentals=0
        ),
        name="swap_lanes",
    )(out)


def shards(occurrence, block_owner, read_block, slot_order):
    devices = lax.axis_size("dev")
    blocks = occurrence.shape[0]
    slots = slot_order.shape[1]
    spill = 2 * blocks // devices
    early, late, kept, cross = lane_sizes(blocks, devices)
    swap = [(d, d ^ 1) for d in range(devices)]
    across = [(d, (d + devices // HALVES) % devices) for d in range(devices)]
    row = jnp.stack([jnp.pad(block_owner[:, 0], (0, slots - blocks)), slot_order[0]])
    everyone = gather_rows(row)
    everyone, mine = lax.optimization_barrier((everyone, occurrence))
    far = lax.ppermute(mine[:kept], "dev", across)
    sibling = lax.ppermute(mine, "dev", swap)
    table = group_table(everyone[:, 0, :blocks], everyone[:, 1])
    cross_send, sends, pick = plan(table, blocks, early, late, kept, cross)
    full = too_full(table, blocks, early, late, kept, cross)
    crossing, out = pack((cross_send, sends[0]), (mine, sibling))
    crossed = lax.ppermute(crossing, "dev", across)
    got = swap_lanes(out, early, 1)
    far, crossed, got = lax.optimization_barrier((far, crossed, got))
    near = (mine, sibling, far, lax.ppermute(far, "dev", swap))
    near = near + (crossed, lax.ppermute(crossed, "dev", swap))
    also = swap_lanes(pack((sends[1],), near)[0], late, 2)
    first = tiles(pick, read_block, near + (got, also))

    def more(carry):
        begin, stop, margin = carry
        begin, now, mine = lax.optimization_barrier((begin, table, occurrence))
        send, pick, local = routes(now, blocks)
        sibling = lax.ppermute(mine, "dev", swap)
        far = lax.ppermute(mine, "dev", across)
        near = (mine, sibling, far, lax.ppermute(far, "dev", swap))
        got = exchange(pack((send(begin, spill, False),), near[:CORES])[0], spill)
        also = exchange(pack((send(begin, spill, True),), near[CORES:])[0], spill)
        added = tiles(pick(begin, spill, local), read_block, near + (got, also))
        margin = jnp.where(begin == 0, 0.0, margin) + added
        return begin + CORES * spill, i32(fullest_lane(now, blocks)), margin

    start = jnp.int32(0), jnp.where(full, 1, 0).astype(jnp.int32), first
    return lax.while_loop(lambda carry: carry[0] < carry[1], more, start)[2]


def solution(mesh):
    placed = (P("dev", None, None), P("dev", None), P("dev"), P("dev", None))
    return jax.shard_map(
        shards, mesh=mesh, in_specs=placed, out_specs=P("dev", None), check_vma=False
    )
```

```python
import functools
import jax
import jax.numpy as jnp
import numpy as np
from jax import lax
from jax.experimental import pallas as pl
from jax.experimental.pallas import tpu as pltpu
from jax.sharding import PartitionSpec as P

CAP = 4
RB_DEV = 16
CORES = 2
HALVES = 2
FAMILY = CORES * HALVES
AHEAD = 4
TOGETHER = 4


def i32(x):
    return x.astype(jnp.int32)


def iota(*shape, axis):
    return lax.broadcasted_iota(jnp.int32, shape, axis)


def group_table(owners, order):
    devices, blocks = owners.shape
    slots = order.shape[1]
    per_pair = slots // devices
    earlier = iota(blocks, blocks, axis=1) < iota(blocks, blocks, axis=0)
    same = owners[:, :, None] == owners[:, None, :]
    rank = jnp.sum(i32(same & earlier[None]), axis=2)
    key = owners * per_pair + rank
    number = iota(devices, blocks, axis=0) * blocks + iota(devices, blocks, axis=1) + 1
    hit = key[:, :, None] == iota(1, 1, slots, axis=2)
    holder = jnp.sum(jnp.where(hit, number[:, :, None], 0), axis=1)
    holder = holder.reshape(devices, devices, per_pair).transpose(1, 0, 2).reshape(devices, slots)
    turned = order.reshape(devices, slots // CAP, CAP).transpose(2, 0, 1)
    hit = turned[:, :, :, None] == iota(1, 1, 1, slots, axis=3)
    table = jnp.sum(jnp.where(hit, holder[None, :, None, :], 0), axis=3)
    return table.reshape(CAP, devices * slots // CAP)


def fullest_lane(table, blocks):
    devices = lax.axis_size("dev")
    families = devices // FAMILY
    chips = devices // CORES
    source = jnp.where(table > 0, (table - 1) // blocks, -1)
    named = source[:, :, None] == iota(1, 1, devices, axis=2)
    held = jnp.sum(i32(named), axis=0)
    held_chip = jnp.sum(held.reshape(-1, chips, CORES), axis=2)
    demand = jnp.einsum(
        "gc,gd->cd",
        held_chip.astype(jnp.bfloat16),
        (held > 0).astype(jnp.bfloat16),
        preferred_element_type=jnp.float32,
    )
    c, d = iota(chips, devices, axis=0), iota(chips, devices, axis=1)
    return jnp.max(jnp.where(c % families != d // CORES % families, demand, 0.0))


def routes(table, blocks):
    devices = lax.axis_size("dev")
    families = devices // FAMILY
    half_devices = devices // HALVES
    many = FAMILY * blocks
    me = lax.axis_index("dev")
    half, family, core = me // half_devices, me // CORES % families, me % CORES
    x = jnp.arange(many, dtype=jnp.int32)
    x_half, x_core, x_block = x // (CORES * blocks), x // blocks % CORES, x % blocks
    ids = (((x_half * families + family) * CORES + x_core) * blocks + x_block + 1)[:, None]
    inside = (table[0][None] == ids) | (table[1][None] == ids)
    for j in range(2, CAP):
        inside = inside | (table[j][None] == ids)
    partners = jnp.stack(
        [jnp.sum(jnp.where(inside, table[j][None], 0), axis=1) for j in range(CAP)]
    )
    source = jnp.where(partners > 0, (partners - 1) // blocks, -1)
    target = iota(1, half_devices, axis=1) + half * half_devices
    named = source[:, :, None] == target[None]
    need = jnp.any(named, axis=0) & (target // CORES % families != family)
    row, column = iota(many, many, axis=0), iota(many, many, axis=1)
    same_chip = row // (CORES * blocks) == column // (CORES * blocks)
    before = ((column < row) & same_chip).astype(jnp.bfloat16)
    rank = i32(jnp.dot(before, need.astype(jnp.bfloat16), preferred_element_type=jnp.float32))
    rank = jnp.where(need, rank, -1).T
    local = (i32(x_half != half) * CORES + i32(x_core != core)) * blocks + x_block

    begin = half * CORES * blocks + core * blocks
    own = lax.dynamic_slice(partners, (0, begin), (CAP, blocks)).reshape(-1)
    total = devices * blocks
    match = own[:, None] == iota(1, total, axis=1) + 1
    wanted = jnp.any(match, axis=0).reshape(HALVES, families, CORES * blocks)
    wanted = wanted.transpose(1, 0, 2).reshape(families, many)
    arrived = i32(
        jnp.dot(wanted.astype(jnp.bfloat16), before.T, preferred_element_type=jnp.float32)
    )
    f = iota(families, many, axis=0)
    part = i32(iota(families, many, axis=1) // (CORES * blocks) != half)

    def send(begin, lane, far):
        spot = begin + iota(1, lane, 1, axis=1) * CORES + core
        chosen = jnp.where((x_half != half) == far, local % (CORES * blocks), 0)
        hit = (rank[:, None, :] == spot) & ((x_half != half) == far)
        return jnp.sum(jnp.where(hit, chosen[None, None, :], 0), axis=2).reshape(-1)

    def pick(begin, lane, local):
        empty = many + HALVES * half_devices * lane
        now = arrived - begin
        there = (part * half_devices + f * CORES + now % CORES) * lane + now // CORES + many
        there = jnp.where((now >= 0) & (now < lane * CORES), there, empty)
        place = jnp.where((f == family) & (begin == 0), local[None, :], jnp.where(f == family, empty, there))
        place = place.reshape(families, HALVES, CORES * blocks).transpose(1, 0, 2).reshape(1, total)
        found = jnp.sum(jnp.where(match, place, 0), axis=1)
        return jnp.where(own > 0, found, empty)

    return send, pick, local


def lane_sizes(blocks, devices):
    share = max(1, CORES * blocks * CORES // devices)
    early, late = CORES * ((9 * share + 7) // 8), CORES * ((7 * share + 3) // 4)
    kept = blocks // 4
    cross = 37 * (CORES * (blocks - kept)) // 48
    return early, late, kept, cross - cross % CORES


def chip_counts(table, blocks, kept):
    devices = lax.axis_size("dev")
    chips = devices // CORES
    source = jnp.where(table > 0, (table - 1) // (blocks * CORES), -1)
    spot = (table - 1) % blocks
    named = source[:, :, None] == iota(1, 1, chips, axis=2)
    held = jnp.sum(i32(named), axis=0)
    packed = jnp.sum(i32(named & (spot >= kept)[:, :, None]), axis=0)
    return held, packed


def too_full(table, blocks, early, late, kept, cross):
    devices = lax.axis_size("dev")
    chips = devices // CORES
    families = devices // FAMILY
    held, packed = chip_counts(table, blocks, kept)
    here = (held > 0).astype(jnp.bfloat16)
    demand = jnp.einsum(
        "gc,gd->cd", held.astype(jnp.bfloat16), here, preferred_element_type=jnp.float32
    )
    c, d = iota(chips, chips, axis=0), iota(chips, chips, axis=1)
    near = jnp.where(c // families == d // families, demand, 0.0)
    far = jnp.where(c // families != d // families, demand, 0.0)
    other = jnp.concatenate([far[families:], far[:families]], axis=0)
    load = other + jnp.maximum(near - early, 0.0)
    load = jnp.max(jnp.where(c % families != d % families, load, 0.0))
    halves = jnp.max(here.reshape(-1, HALVES, families), axis=2)
    crossing = jnp.einsum(
        "gc,gh->ch", packed.astype(jnp.bfloat16), halves, preferred_element_type=jnp.float32
    )
    c, h = iota(chips, HALVES, axis=0), iota(chips, HALVES, axis=1)
    crossing = jnp.max(jnp.where(c // families != h, crossing, 0.0))
    return (load > late) | (crossing > cross)


def orders_of(blocks, kept):
    devices = lax.axis_size("dev")
    families = devices // FAMILY
    me = lax.axis_index("dev")
    half, family, core = me // (devices // HALVES), me // CORES % families, me % CORES
    part = np.repeat(np.arange(HALVES), CORES * blocks)
    x_core = np.tile(np.repeat(np.arange(CORES), blocks), HALVES)
    x_block = np.tile(np.arange(blocks), FAMILY)
    order = np.lexsort((x_block, x_core, (part == 1) & (x_block >= kept), part))
    part, x_core, x_block = (jnp.asarray(v[order], jnp.int32) for v in (part, x_core, x_block))
    return half, family, core, part, x_core, x_block


def plan(table, blocks, early, late, kept, cross):
    devices = lax.axis_size("dev")
    families = devices // FAMILY
    many = FAMILY * blocks
    pair = CORES * blocks
    half, family, core, part, x_core, x_block = orders_of(blocks, kept)
    x_half = jnp.where(half == 0, part, 1 - part)
    away = jnp.where(core == 0, x_core, 1 - x_core)

    ids = (((x_half * families + family) * CORES + x_core) * blocks + x_block + 1)[:, None]
    inside = (table[0][None] == ids) | (table[1][None] == ids)
    for j in range(2, CAP):
        inside = inside | (table[j][None] == ids)
    partners = jnp.stack(
        [jnp.sum(jnp.where(inside, table[j][None], 0), axis=1) for j in range(CAP)]
    )
    chip = jnp.where(partners > 0, (partners - 1) // pair, -1)
    mask = iota(1, families, axis=1)
    target = (family ^ mask) + half * families
    need = jnp.any(chip[:, :, None] == target[None], axis=0) & (mask > 0)
    crosses = jnp.any((partners > 0) & (chip // families != x_half[None]), axis=0)
    crosses = crosses & (x_block >= kept)
    leaves, comes = crosses & (part == 0), crosses & (part == 1)
    wide = jnp.concatenate([need, leaves[:, None], comes[:, None]], axis=1)
    before = (iota(many, many, axis=1) < iota(many, many, axis=0)).astype(jnp.bfloat16)
    ranks = i32(jnp.dot(before, wide.astype(jnp.bfloat16), preferred_element_type=jnp.float32))
    ranks = jnp.where(wide, ranks, -1).T
    rank, leaving, coming = ranks[:families], ranks[families], ranks[families + 1]
    side = cross // CORES
    second = i32(coming >= side)
    packed = pair + CORES * kept
    packed = packed + jnp.where(core == 0, second, 1 - second) * side + coming - second * side
    local = jnp.where(
        part == 0,
        away * blocks + x_block,
        jnp.where(x_block < kept, pair + away * kept + x_block, packed),
    )

    spots = iota(1, side, 1, axis=1)[0] + core * side
    cross_send = jnp.sum(jnp.where(leaving[None] == spots, local[None], 0), axis=1)

    def send(first, lane):
        spot = first[:, None, None] + iota(1, lane // CORES, 1, axis=1) + core * (lane // CORES)
        hit = (rank[:, None, :] == spot) & (part == 0)
        return jnp.sum(jnp.where(hit, local[None, None, :], 0), axis=2).reshape(-1)

    zero = jnp.zeros((families,), jnp.int32)
    return cross_send, send(zero, early), (partners, rank, need, local)


def late_plan(known, blocks, early, late, kept, cross):
    partners, rank, need, local = known
    devices = lax.axis_size("dev")
    families = devices // FAMILY
    many = FAMILY * blocks
    pair = CORES * blocks
    half, family, core, part, x_core, x_block = orders_of(blocks, kept)
    x_half = jnp.where(half == 0, part, 1 - part)
    near_count = jnp.sum(i32(need & (part == 0)[:, None]), axis=0)
    shipped = jnp.minimum(near_count, early)
    side = late // CORES
    spot = shipped[:, None, None] + iota(1, side, 1, axis=1) + core * side
    hit = rank[:, None, :] == spot
    then = jnp.sum(jnp.where(hit, local[None, None, :], 0), axis=2).reshape(-1)

    mask = iota(families, 1, axis=0)
    pairs = partners[:, :pair].reshape(-1)
    all_ids = (
        ((x_half[None] * families + (family ^ mask)) * CORES + x_core[None]) * blocks
        + x_block[None]
        + 1
    ).reshape(1, -1)
    wanted = jnp.any(pairs[:, None] == all_ids, axis=0).reshape(families, many)
    before = (iota(many, many, axis=0) < iota(many, many, axis=1)).astype(jnp.bfloat16)
    arrived = i32(
        jnp.dot(wanted.astype(jnp.bfloat16), before, preferred_element_type=jnp.float32)
    )
    came = jnp.sum(i32(wanted & (part == 0)[None]), axis=1, keepdims=True)
    came = jnp.minimum(came, early)
    base = pair + CORES * kept + cross
    place = jnp.where(
        arrived < came,
        base + mask * early + arrived,
        base + families * early + mask * late + arrived - came,
    )
    place = jnp.where(mask == 0, local[None], place).reshape(1, -1)
    empty = base + families * (early + late)
    own = lax.dynamic_slice(partners, (0, core * blocks), (CAP, blocks)).reshape(-1)
    picked = jnp.sum(jnp.where(own[:, None] == all_ids, place, 0), axis=1)
    return then, jnp.where(own > 0, picked, empty)


def fill(refs, held, sems):
    copies, at = [], 0
    for i, ref in enumerate(refs):
        copies.append(
            pltpu.make_async_copy(ref, held.at[pl.ds(at, ref.shape[0])], sems.at[i])
        )
        copies[-1].start()
        at += ref.shape[0]
    return copies


def pack_kernel(parts, send_ref, *refs):
    near, outs, (held, sems) = refs[: -2 - parts], refs[-2 - parts : -2], refs[-2:]
    for copy in fill(near, held, sems):
        copy.wait()
    begin = 0
    for out_ref in outs:

        def step(i, _):
            out_ref[i] = held[send_ref[begin + i]]
            return 0

        lax.fori_loop(0, out_ref.shape[0], step, 0, unroll=2)
        begin += out_ref.shape[0]


def tile_kernel(pick_ref, read_ref, *refs):
    near, (out_ref, held, sems) = refs[:-3], refs[-3:]
    blocks, rows = near[0].shape[:2]
    copies = fill(near, held, sems)
    held[held.shape[0] - 1] = jnp.zeros(held.shape[1:], held.dtype)
    out_ref[...] = jnp.zeros_like(out_ref)
    for copy in copies:
        copy.wait()

    def tile_of(b):
        others = jnp.concatenate([held[pick_ref[j * blocks + b]] for j in range(CAP)], axis=0)
        tile = lax.dot_general(
            held[b], others, (((1,), (1,)), ((), ())), preferred_element_type=jnp.float32
        )
        return tile.astype(jnp.bfloat16)

    def step(i, _):
        found = [tile_of(i * TOGETHER + k) for k in range(TOGETHER)]
        for k in range(TOGETHER):
            begin = read_ref[i * TOGETHER + k] * rows
            where = pl.ds(pl.multiple_of(begin, rows), rows)
            out_ref[where, :] += found[k].astype(jnp.float32)
        return 0

    lax.fori_loop(0, blocks // TOGETHER, step, 0, unroll=2)


SMEM = pl.BlockSpec(memory_space=pltpu.SMEM)
HBM = pl.BlockSpec(memory_space=pl.ANY)
VMEM = pl.BlockSpec(memory_space=pltpu.VMEM)


def pack(send, near, lanes=None):
    rows, kmers = near[0].shape[1:]
    total = sum(ref.shape[0] for ref in near)
    lanes = lanes or [send.shape[0]]
    return pl.pallas_call(
        functools.partial(pack_kernel, len(lanes)),
        out_shape=[jax.ShapeDtypeStruct((lane, rows, kmers), near[0].dtype) for lane in lanes],
        in_specs=[SMEM] + [HBM] * len(near),
        out_specs=[VMEM] * len(lanes),
        scratch_shapes=[
            pltpu.VMEM((total, rows, kmers), near[0].dtype),
            pltpu.SemaphoreType.DMA((len(near),)),
        ],
        compiler_params=pltpu.CompilerParams(vmem_limit_bytes=60 << 20),
        name="pack",
    )(send, *near)


def tiles(pick, read_block, near):
    rows, kmers = near[0].shape[1:]
    total = sum(ref.shape[0] for ref in near) + 1
    return pl.pallas_call(
        tile_kernel,
        out_shape=jax.ShapeDtypeStruct((RB_DEV * rows, CAP * rows), jnp.float32),
        in_specs=[SMEM, SMEM] + [HBM] * len(near),
        out_specs=VMEM,
        scratch_shapes=[
            pltpu.VMEM((total, rows, kmers), near[0].dtype),
            pltpu.SemaphoreType.DMA((len(near),)),
        ],
        compiler_params=pltpu.CompilerParams(vmem_limit_bytes=60 << 20),
        name="tiles",
    )(pick, read_block, *near)


def greet(others):
    barrier = pltpu.get_barrier_semaphore()
    for other in others:
        pl.semaphore_signal(
            barrier, inc=1, device_id=(other,), device_id_type=pl.DeviceIdType.MESH
        )
    pl.semaphore_wait(barrier, len(others))


def everyone_kernel(
    devices, row_ref, mine_ref, owners_ref, orders_ref, sibling_ref, lead_ref, got, lead, *sems
):
    send_sems, recv_sems, move_sems = sems
    me = lax.axis_index("dev")
    load = pltpu.make_async_copy(mine_ref.at[pl.ds(0, lead.shape[0])], lead, move_sems.at[0])
    load.start()
    got[me] = row_ref[...]
    greet([(me + k) % devices for k in range(1, devices)])
    copies = [
        pltpu.make_async_remote_copy(
            src_ref=row_ref,
            dst_ref=got.at[me],
            send_sem=send_sems.at[k],
            recv_sem=recv_sems.at[k],
            device_id=((me + k) % devices,),
            device_id_type=pl.DeviceIdType.MESH,
        )
        for k in range(1, devices)
    ]
    for copy in copies:
        copy.start()
    swap = pltpu.make_async_remote_copy(
        src_ref=mine_ref,
        dst_ref=sibling_ref,
        send_sem=send_sems.at[0],
        recv_sem=recv_sems.at[0],
        device_id=(me + 1 - 2 * (me % CORES),),
        device_id_type=pl.DeviceIdType.MESH,
    )
    swap.start()
    load.wait()
    store = pltpu.make_async_copy(lead, lead_ref, move_sems.at[1])
    store.start()
    for copy in copies:
        copy.wait()
    owners_ref[...] = got[:, 0, :]
    orders_ref[...] = got[:, 1, :]
    store.wait()
    swap.wait()


def gather_rows(row, mine, kept):
    devices = lax.axis_size("dev")
    slots = row.shape[1]
    table = jax.ShapeDtypeStruct((devices, slots), row.dtype)
    lead = (kept,) + mine.shape[1:]
    return pl.pallas_call(
        functools.partial(everyone_kernel, devices),
        out_shape=[
            table,
            table,
            jax.ShapeDtypeStruct(mine.shape, mine.dtype),
            jax.ShapeDtypeStruct(lead, mine.dtype),
        ],
        in_specs=[VMEM, HBM],
        out_specs=[VMEM, VMEM, HBM, HBM],
        scratch_shapes=[
            pltpu.VMEM((devices,) + row.shape, row.dtype),
            pltpu.VMEM(lead, mine.dtype),
            pltpu.SemaphoreType.DMA((devices,)),
            pltpu.SemaphoreType.DMA((devices,)),
            pltpu.SemaphoreType.DMA((2,)),
        ],
        compiler_params=pltpu.CompilerParams(has_side_effects=True, collective_id=0),
        name="gather_rows",
    )(row, mine)


def flipped(value, mask):
    bit = 1
    while bit <= mask:
        if mask & bit:
            value = value + bit - 2 * bit * (value // bit % 2)
        bit *= 2
    return value


def exchange_kernel(devices, lane, out_ref, got_ref, send_sems, recv_sems):
    me = lax.axis_index("dev")
    count = devices // HALVES
    spot = me % count

    def copy_of(k):
        to = flipped(spot, k)
        return pltpu.make_async_remote_copy(
            src_ref=out_ref.at[pl.ds(to * lane, lane)],
            dst_ref=got_ref.at[pl.ds(spot * lane, lane)],
            send_sem=send_sems.at[k],
            recv_sem=recv_sems.at[k],
            device_id=(me - spot + to,),
            device_id_type=pl.DeviceIdType.MESH,
        )

    chips = count // CORES
    steps = []
    for mask in range(chips - 1, chips // 2 - 1, -1):
        for core in range(CORES):
            masks = [m for m in (mask, chips - 1 - mask) if m]
            steps.append([copy_of(m * CORES + core) for m in masks])
    for i, step in enumerate(steps):
        if i >= 2:
            for copy in steps[i - 2]:
                copy.wait_send()
        for copy in step:
            copy.start()
    for step in steps[-2:]:
        for copy in step:
            copy.wait_send()
    for step in steps:
        for copy in step:
            copy.wait_recv()


def exchange(out, lane):
    devices = lax.axis_size("dev")
    count = devices // HALVES
    return pl.pallas_call(
        functools.partial(exchange_kernel, devices, lane),
        out_shape=jax.ShapeDtypeStruct(out.shape, out.dtype),
        in_specs=[HBM],
        out_specs=HBM,
        scratch_shapes=[pltpu.SemaphoreType.DMA((count,))] * 2,
        compiler_params=pltpu.CompilerParams(has_side_effects=True),
        cost_estimate=pl.CostEstimate(
            flops=0, bytes_accessed=32 * out.size * out.dtype.itemsize, transcendentals=0
        ),
        name="exchange",
    )(out)


def trade_kernel(devices, early, late, cuts, *refs):
    then_ref, mine_ref, sibling_ref, far_ref, cross_ref, out_ref = refs[:6]
    got_ref, also_ref, far_twin_ref, own_ref, twin_ref, held, lanes = refs[6:13]
    fill_sems, cross_sems, soon_sems, last_sems = refs[13:]
    families = devices // FAMILY
    me = lax.axis_index("dev")
    chip, core = me // CORES, me % CORES
    spot = chip % families
    twin, opposite = chip * CORES + 1 - core, (me + devices // HALVES) % devices
    blocks, kept, side = mine_ref.shape[0], far_ref.shape[0], cross_ref.shape[0]
    at = {"far": CORES * blocks, "far_twin": CORES * blocks + kept}
    at["own"] = CORES * blocks + CORES * kept
    at["twin"] = at["own"] + side

    def part(name, begin, size):
        return held.at[pl.ds(at[name] + begin, size)]

    def remote(src, dst, send_sem, recv_sem, to):
        return pltpu.make_async_remote_copy(
            src_ref=src,
            dst_ref=dst,
            send_sem=send_sem,
            recv_sem=recv_sem,
            device_id=(to,),
            device_id_type=pl.DeviceIdType.MESH,
        )

    fills = [
        pltpu.make_async_copy(mine_ref, held.at[pl.ds(0, blocks)], fill_sems.at[0]),
        pltpu.make_async_copy(sibling_ref, held.at[pl.ds(blocks, blocks)], fill_sems.at[1]),
        pltpu.make_async_copy(far_ref, part("far", 0, kept), fill_sems.at[2]),
    ]
    for copy in fills:
        copy.start()
    chips = {k: (chip - spot + flipped(spot, k)) * CORES + core for k in range(1, families)}
    greet(list(chips.values()) + [twin, opposite])

    crossing, passing = [], []
    for i, (begin, size) in enumerate(cuts):
        here = part("own", begin, size)
        crossing.append(
            remote(
                cross_ref.at[pl.ds(begin, size)],
                here,
                cross_sems.at[4 * i],
                cross_sems.at[4 * i + 1],
                opposite,
            )
        )
        passing.append(
            remote(
                here,
                part("twin", begin, size),
                cross_sems.at[4 * i + 2],
                cross_sems.at[4 * i + 3],
                twin,
            )
        )
    last = 4 * len(cuts)
    share = remote(
        far_ref, part("far_twin", 0, kept), cross_sems.at[last], cross_sems.at[last + 1], twin
    )
    for copy in crossing:
        copy.start()
    share.start()

    top = families - 1
    steps = [[k for k in (m, top - m) if k] for m in range(top, families // 2 - 1, -1)]

    def lanes_of(src_ref, dst_ref, lane, sems):
        size = lane // CORES
        sent, passed = [], []
        for step in steps:
            sent.append([])
            passed.append([])
            for k in step:
                begin = k * lane + core * size
                rows = dst_ref.at[pl.ds(begin, size)]
                src = src_ref.at[pl.ds(k * size, size)]
                sent[-1].append(remote(src, rows, sems.at[4 * k], sems.at[4 * k + 1], chips[k]))
                passed[-1].append(
                    remote(rows, rows, sems.at[4 * k + 2], sems.at[4 * k + 3], twin)
                )
        return sent, passed

    def start(sent, i):
        for copy in sent[i]:
            copy.start()

    def finish(sent, i):
        for copy in sent[i]:
            copy.wait_send()

    def land(sent, passed, i):
        for copy, follow in zip(sent[i], passed[i]):
            copy.wait_recv()
            follow.start()

    count = len(steps)
    ahead = min(AHEAD, count)
    soon, soon_passed = lanes_of(out_ref, got_ref, early, soon_sems)
    for i in range(count):
        if i >= ahead:
            finish(soon, i - ahead)
        start(soon, i)
        if i >= ahead:
            land(soon, soon_passed, i - ahead)

    for copy, follow in zip(crossing, passing):
        copy.wait_recv()
        follow.start()
    for copy in fills:
        copy.wait()
    share.wait_recv()
    for follow in passing:
        follow.wait_recv()
    stores = [
        pltpu.make_async_copy(part("far_twin", 0, kept), far_twin_ref, fill_sems.at[3]),
        pltpu.make_async_copy(part("own", 0, side), own_ref, fill_sems.at[4]),
        pltpu.make_async_copy(part("twin", 0, side), twin_ref, fill_sems.at[5]),
    ]
    for copy in stores:
        copy.start()

    size = late // CORES
    for step in steps:
        for k in step:

            def move(i, _):
                lanes[k * size + i] = held[then_ref[k * size + i]]
                return 0

            lax.fori_loop(0, size, move, 0, unroll=2)

    late_sent, late_passed = lanes_of(lanes, also_ref, late, last_sems)
    for i in range(ahead):
        start(late_sent, i)
    for i in range(count - ahead, count):
        finish(soon, i)
        land(soon, soon_passed, i)
    for i in range(ahead, count):
        finish(late_sent, i - ahead)
        start(late_sent, i)
        land(late_sent, late_passed, i - ahead)
    for i in range(count - ahead, count):
        finish(late_sent, i)
        land(late_sent, late_passed, i)
    for copy in crossing + passing + [share]:
        copy.wait_send()
    for copy in stores:
        copy.wait()
    for step in soon_passed + late_passed:
        for follow in step:
            follow.wait()


def trade(then, mine, sibling, far, crossing, out, early, late):
    devices = lax.axis_size("dev")
    families = devices // FAMILY
    shape, kind = mine.shape[1:], mine.dtype
    kept, side = far.shape[0], crossing.shape[0]
    cuts = [(0, side // 2), (side // 2, side - side // 2)]
    held = CORES * (mine.shape[0] + kept + side)

    def rows(count):
        return jax.ShapeDtypeStruct((count,) + shape, kind)

    return pl.pallas_call(
        functools.partial(trade_kernel, devices, early, late, cuts),
        out_shape=[
            rows(families * early),
            rows(families * late),
            rows(kept),
            rows(side),
            rows(side),
        ],
        in_specs=[SMEM] + [HBM] * 5,
        out_specs=[HBM] * 5,
        scratch_shapes=[
            pltpu.VMEM((held,) + shape, kind),
            pltpu.VMEM((families * late // CORES,) + shape, kind),
            pltpu.SemaphoreType.DMA((6,)),
            pltpu.SemaphoreType.DMA((4 * len(cuts) + 2,)),
            pltpu.SemaphoreType.DMA((4 * families,)),
            pltpu.SemaphoreType.DMA((4 * families,)),
        ],
        compiler_params=pltpu.CompilerParams(
            has_side_effects=True, collective_id=1, vmem_limit_bytes=60 << 20
        ),
        name="trade",
    )(then, mine, sibling, far, crossing, out)


def shards(occurrence, block_owner, read_block, slot_order):
    devices = lax.axis_size("dev")
    blocks = occurrence.shape[0]
    slots = slot_order.shape[1]
    spill = 2 * blocks // devices
    early, late, kept, cross = lane_sizes(blocks, devices)
    swap = [(d, d ^ 1) for d in range(devices)]
    across = [(d, (d + devices // HALVES) % devices) for d in range(devices)]
    row = jnp.stack([jnp.pad(block_owner[:, 0], (0, slots - blocks)), slot_order[0]])
    mine = occurrence
    owners, orders, sibling, lead = gather_rows(row, mine, kept)
    far = lax.ppermute(lead, "dev", across)
    table = group_table(owners[:, :blocks], orders)
    sizes = blocks, early, late, kept, cross
    cross_send, send, known = plan(table, *sizes)
    lanes = cross // CORES, send.shape[0]
    crossing, out = pack(jnp.concatenate([cross_send, send]), (mine, sibling), lanes)
    then, pick = late_plan(known, *sizes)
    full = too_full(table, *sizes)
    far, then, pick, full = lax.optimization_barrier((far, then, pick, full))
    got, also, far_twin, own, twin = trade(then, mine, sibling, far, crossing, out, early, late)
    first = tiles(pick, read_block, (mine, sibling, far, far_twin, own, twin, got, also))

    def more(carry):
        begin, _, margin = carry
        begin, now, mine = lax.optimization_barrier((begin, table, occurrence))
        send, pick, local = routes(now, blocks)
        sibling = lax.ppermute(mine, "dev", swap)
        far = lax.ppermute(mine, "dev", across)
        near = (mine, sibling, far, lax.ppermute(far, "dev", swap))
        got = exchange(pack(send(begin, spill, False), near[:CORES])[0], spill)
        also = exchange(pack(send(begin, spill, True), near[CORES:])[0], spill)
        added = tiles(pick(begin, spill, local), read_block, near + (got, also))
        margin = jnp.where(begin == 0, 0.0, margin) + added
        return begin + CORES * spill, i32(fullest_lane(now, blocks)), margin

    start = jnp.int32(0), jnp.where(full, 1, 0).astype(jnp.int32), first
    return lax.while_loop(lambda carry: carry[0] < carry[1], more, start)[2]


def solution(mesh):
    placed = (P("dev", None, None), P("dev", None), P("dev"), P("dev", None))
    return jax.shard_map(
        shards, mesh=mesh, in_specs=placed, out_specs=P("dev", None), check_vma=False
    )
```

```python
import functools
import jax
import jax.numpy as jnp
import numpy as np
from jax import lax
from jax.experimental import pallas as pl
from jax.experimental.pallas import tpu as pltpu
from jax.sharding import PartitionSpec as P

CAP = 4
RB_DEV = 16
CORES = 2
HALVES = 2
FAMILY = CORES * HALVES
AHEAD = 4, 4
TOGETHER = 4


def i32(x):
    return x.astype(jnp.int32)


def iota(*shape, axis):
    return lax.broadcasted_iota(jnp.int32, shape, axis)


def group_table(owners, order):
    devices, blocks = owners.shape
    slots = order.shape[1]
    per_pair = slots // devices
    earlier = iota(blocks, blocks, axis=1) < iota(blocks, blocks, axis=0)
    same = owners[:, :, None] == owners[:, None, :]
    rank = jnp.sum(i32(same & earlier[None]), axis=2)
    key = owners * per_pair + rank
    number = iota(devices, blocks, axis=0) * blocks + iota(devices, blocks, axis=1) + 1
    hit = key[:, :, None] == iota(1, 1, slots, axis=2)
    holder = jnp.sum(jnp.where(hit, number[:, :, None], 0), axis=1)
    holder = holder.reshape(devices, devices, per_pair).transpose(1, 0, 2).reshape(devices, slots)
    turned = order.reshape(devices, slots // CAP, CAP).transpose(2, 0, 1)
    hit = turned[:, :, :, None] == iota(1, 1, 1, slots, axis=3)
    table = jnp.sum(jnp.where(hit, holder[None, :, None, :], 0), axis=3)
    return table.reshape(CAP, devices * slots // CAP)


def fullest_lane(table, blocks):
    devices = lax.axis_size("dev")
    families = devices // FAMILY
    chips = devices // CORES
    source = jnp.where(table > 0, (table - 1) // blocks, -1)
    named = source[:, :, None] == iota(1, 1, devices, axis=2)
    held = jnp.sum(i32(named), axis=0)
    held_chip = jnp.sum(held.reshape(-1, chips, CORES), axis=2)
    demand = jnp.einsum(
        "gc,gd->cd",
        held_chip.astype(jnp.bfloat16),
        (held > 0).astype(jnp.bfloat16),
        preferred_element_type=jnp.float32,
    )
    c, d = iota(chips, devices, axis=0), iota(chips, devices, axis=1)
    return jnp.max(jnp.where(c % families != d // CORES % families, demand, 0.0))


def routes(table, blocks):
    devices = lax.axis_size("dev")
    families = devices // FAMILY
    half_devices = devices // HALVES
    many = FAMILY * blocks
    me = lax.axis_index("dev")
    half, family, core = me // half_devices, me // CORES % families, me % CORES
    x = jnp.arange(many, dtype=jnp.int32)
    x_half, x_core, x_block = x // (CORES * blocks), x // blocks % CORES, x % blocks
    ids = (((x_half * families + family) * CORES + x_core) * blocks + x_block + 1)[:, None]
    inside = (table[0][None] == ids) | (table[1][None] == ids)
    for j in range(2, CAP):
        inside = inside | (table[j][None] == ids)
    partners = jnp.stack(
        [jnp.sum(jnp.where(inside, table[j][None], 0), axis=1) for j in range(CAP)]
    )
    source = jnp.where(partners > 0, (partners - 1) // blocks, -1)
    target = iota(1, half_devices, axis=1) + half * half_devices
    named = source[:, :, None] == target[None]
    need = jnp.any(named, axis=0) & (target // CORES % families != family)
    row, column = iota(many, many, axis=0), iota(many, many, axis=1)
    same_chip = row // (CORES * blocks) == column // (CORES * blocks)
    before = ((column < row) & same_chip).astype(jnp.bfloat16)
    rank = i32(jnp.dot(before, need.astype(jnp.bfloat16), preferred_element_type=jnp.float32))
    rank = jnp.where(need, rank, -1).T
    local = (i32(x_half != half) * CORES + i32(x_core != core)) * blocks + x_block

    begin = half * CORES * blocks + core * blocks
    own = lax.dynamic_slice(partners, (0, begin), (CAP, blocks)).reshape(-1)
    total = devices * blocks
    match = own[:, None] == iota(1, total, axis=1) + 1
    wanted = jnp.any(match, axis=0).reshape(HALVES, families, CORES * blocks)
    wanted = wanted.transpose(1, 0, 2).reshape(families, many)
    arrived = i32(
        jnp.dot(wanted.astype(jnp.bfloat16), before.T, preferred_element_type=jnp.float32)
    )
    f = iota(families, many, axis=0)
    part = i32(iota(families, many, axis=1) // (CORES * blocks) != half)

    def send(begin, lane, far):
        spot = begin + iota(1, lane, 1, axis=1) * CORES + core
        chosen = jnp.where((x_half != half) == far, local % (CORES * blocks), 0)
        hit = (rank[:, None, :] == spot) & ((x_half != half) == far)
        return jnp.sum(jnp.where(hit, chosen[None, None, :], 0), axis=2).reshape(-1)

    def pick(begin, lane, local):
        empty = many + HALVES * half_devices * lane
        now = arrived - begin
        there = (part * half_devices + f * CORES + now % CORES) * lane + now // CORES + many
        there = jnp.where((now >= 0) & (now < lane * CORES), there, empty)
        place = jnp.where((f == family) & (begin == 0), local[None, :], jnp.where(f == family, empty, there))
        place = place.reshape(families, HALVES, CORES * blocks).transpose(1, 0, 2).reshape(1, total)
        found = jnp.sum(jnp.where(match, place, 0), axis=1)
        return jnp.where(own > 0, found, empty)

    return send, pick, local


def lane_sizes(blocks, devices):
    share = max(1, CORES * blocks * CORES // devices)
    soon, rest = 2.1 * share, 1.26 * share
    early = CORES * round((soon + 0.8 * soon**0.5) / CORES)
    late = CORES * round((rest + 4.4 * rest**0.5) / CORES)
    kept = blocks // 4
    cross = 37 * (CORES * (blocks - kept)) // 48
    return early, late, kept, cross - cross % CORES


def chip_counts(table, blocks, kept):
    devices = lax.axis_size("dev")
    chips = devices // CORES
    source = jnp.where(table > 0, (table - 1) // (blocks * CORES), -1)
    spot = (table - 1) % blocks
    named = source[:, :, None] == iota(1, 1, chips, axis=2)
    held = jnp.sum(i32(named), axis=0)
    packed = jnp.sum(i32(named & (spot >= kept)[:, :, None]), axis=0)
    return held, packed


def too_full(table, blocks, early, late, kept, cross):
    devices = lax.axis_size("dev")
    chips = devices // CORES
    families = devices // FAMILY
    held, packed = chip_counts(table, blocks, kept)
    here = (held > 0).astype(jnp.bfloat16)
    both = jnp.concatenate([held, packed], axis=1).astype(jnp.bfloat16)
    demand = jnp.einsum("gc,gd->cd", both, here, preferred_element_type=jnp.float32)
    demand, last = demand[:chips], demand[chips:]
    c, d = iota(chips, chips, axis=0), iota(chips, chips, axis=1)
    beyond = c // families != d // families

    def turned(far):
        return jnp.concatenate([far[families:], far[:families]], axis=0)

    last = turned(jnp.where(beyond, last, 0.0))
    soon = jnp.where(beyond, 0.0, demand) + turned(jnp.where(beyond, demand, 0.0)) - last
    load = last + jnp.maximum(soon - early, 0.0)
    load = jnp.max(jnp.where(c % families != d % families, load, 0.0))
    halves = jnp.max(here.reshape(-1, HALVES, families), axis=2)
    crossing = jnp.einsum(
        "gc,gh->ch", packed.astype(jnp.bfloat16), halves, preferred_element_type=jnp.float32
    )
    c, h = iota(chips, HALVES, axis=0), iota(chips, HALVES, axis=1)
    crossing = jnp.max(jnp.where(c // families != h, crossing, 0.0))
    return (load > late) | (crossing > cross)


def orders_of(blocks, kept):
    devices = lax.axis_size("dev")
    families = devices // FAMILY
    me = lax.axis_index("dev")
    half, family, core = me // (devices // HALVES), me // CORES % families, me % CORES
    part = np.repeat(np.arange(HALVES), CORES * blocks)
    x_core = np.tile(np.repeat(np.arange(CORES), blocks), HALVES)
    x_block = np.tile(np.arange(blocks), FAMILY)
    order = np.lexsort((x_block, x_core, (part == 1) & (x_block >= kept), part))
    part, x_core, x_block = (jnp.asarray(v[order], jnp.int32) for v in (part, x_core, x_block))
    return half, family, core, part, x_core, x_block


def plan(table, blocks, early, late, kept, cross):
    devices = lax.axis_size("dev")
    families = devices // FAMILY
    many = FAMILY * blocks
    pair = CORES * blocks
    half, family, core, part, x_core, x_block = orders_of(blocks, kept)
    x_half = jnp.where(half == 0, part, 1 - part)
    away = jnp.where(core == 0, x_core, 1 - x_core)

    ids = (((x_half * families + family) * CORES + x_core) * blocks + x_block + 1)[:, None]
    inside = (table[0][None] == ids) | (table[1][None] == ids)
    for j in range(2, CAP):
        inside = inside | (table[j][None] == ids)
    partners = jnp.stack(
        [jnp.sum(jnp.where(inside, table[j][None], 0), axis=1) for j in range(CAP)]
    )
    chip = jnp.where(partners > 0, (partners - 1) // pair, -1)
    mask = iota(1, families, axis=1)
    target = (family ^ mask) + half * families
    need = jnp.any(chip[:, :, None] == target[None], axis=0) & (mask > 0)
    crosses = jnp.any((partners > 0) & (chip // families != x_half[None]), axis=0)
    crosses = crosses & (x_block >= kept)
    leaves, comes = crosses & (part == 0), crosses & (part == 1)
    wide = jnp.concatenate([need, leaves[:, None], comes[:, None]], axis=1)
    before = (iota(many, many, axis=1) < iota(many, many, axis=0)).astype(jnp.bfloat16)
    ranks = i32(jnp.dot(before, wide.astype(jnp.bfloat16), preferred_element_type=jnp.float32))
    ranks = jnp.where(wide, ranks, -1).T
    rank, leaving, coming = ranks[:families], ranks[families], ranks[families + 1]
    side = cross // CORES
    second = i32(coming >= side)
    packed = pair + CORES * kept
    packed = packed + jnp.where(core == 0, second, 1 - second) * side + coming - second * side
    local = jnp.where(
        part == 0,
        away * blocks + x_block,
        jnp.where(x_block < kept, pair + away * kept + x_block, packed),
    )

    spots = iota(1, side, 1, axis=1)[0] + core * side
    cross_send = jnp.sum(jnp.where(leaving[None] == spots, local[None], 0), axis=1)

    return cross_send, (partners, rank, need, local)


def late_plan(known, blocks, early, late, kept, cross):
    partners, rank, need, local = known
    devices = lax.axis_size("dev")
    families = devices // FAMILY
    many = FAMILY * blocks
    pair = CORES * blocks
    half, family, core, part, x_core, x_block = orders_of(blocks, kept)
    x_half = jnp.where(half == 0, part, 1 - part)
    soon = (part == 0) | (x_block < kept)
    shipped = jnp.minimum(jnp.sum(i32(need & soon[:, None]), axis=0), early)

    def send(first, allowed, side):
        spot = first[:, None, None] + iota(1, side, 1, axis=1) + core * side
        hit = (rank[:, None, :] == spot) & allowed
        return jnp.sum(jnp.where(hit, local[None, None, :], 0), axis=2).reshape(-1)

    sends = send(0 * shipped, soon[None, None, :], early // CORES), send(shipped, True, late // CORES)
    mask = iota(families, 1, axis=0)
    pairs = partners[:, :pair].reshape(-1)
    all_ids = (
        ((x_half[None] * families + (family ^ mask)) * CORES + x_core[None]) * blocks
        + x_block[None]
        + 1
    ).reshape(1, -1)
    wanted = jnp.any(pairs[:, None] == all_ids, axis=0).reshape(families, many)
    before = (iota(many, many, axis=0) < iota(many, many, axis=1)).astype(jnp.bfloat16)
    arrived = i32(
        jnp.dot(wanted.astype(jnp.bfloat16), before, preferred_element_type=jnp.float32)
    )
    came = jnp.sum(i32(wanted & soon[None]), axis=1, keepdims=True)
    came = jnp.minimum(came, early)
    base = pair + CORES * kept + cross
    place = jnp.where(
        arrived < came,
        base + mask * early + arrived,
        base + families * early + mask * late + arrived - came,
    )
    place = jnp.where(mask == 0, local[None], place).reshape(1, -1)
    empty = base + families * (early + late)
    own = lax.dynamic_slice(partners, (0, core * blocks), (CAP, blocks)).reshape(-1)
    picked = jnp.sum(jnp.where(own[:, None] == all_ids, place, 0), axis=1)
    return jnp.concatenate(sends), jnp.where(own > 0, picked, empty)


def fill(refs, held, sems):
    copies, at = [], 0
    for i, ref in enumerate(refs):
        copies.append(
            pltpu.make_async_copy(ref, held.at[pl.ds(at, ref.shape[0])], sems.at[i])
        )
        copies[-1].start()
        at += ref.shape[0]
    return copies


def pack_kernel(parts, send_ref, *refs):
    near, outs, (held, sems) = refs[: -2 - parts], refs[-2 - parts : -2], refs[-2:]
    for copy in fill(near, held, sems):
        copy.wait()
    begin = 0
    for out_ref in outs:

        def step(i, _):
            out_ref[i] = held[send_ref[begin + i]]
            return 0

        lax.fori_loop(0, out_ref.shape[0], step, 0, unroll=2)
        begin += out_ref.shape[0]


def tile_kernel(pick_ref, read_ref, *refs):
    near, (out_ref, held, sems) = refs[:-3], refs[-3:]
    blocks, rows = near[0].shape[:2]
    copies = fill(near, held, sems)
    held[held.shape[0] - 1] = jnp.zeros(held.shape[1:], held.dtype)
    out_ref[...] = jnp.zeros_like(out_ref)
    for copy in copies:
        copy.wait()

    def tile_of(b):
        others = jnp.concatenate([held[pick_ref[j * blocks + b]] for j in range(CAP)], axis=0)
        tile = lax.dot_general(
            held[b], others, (((1,), (1,)), ((), ())), preferred_element_type=jnp.float32
        )
        return tile.astype(jnp.bfloat16)

    def step(i, _):
        found = [tile_of(i * TOGETHER + k) for k in range(TOGETHER)]
        for k in range(TOGETHER):
            begin = read_ref[i * TOGETHER + k] * rows
            where = pl.ds(pl.multiple_of(begin, rows), rows)
            out_ref[where, :] += found[k].astype(jnp.float32)
        return 0

    lax.fori_loop(0, blocks // TOGETHER, step, 0, unroll=2)


SMEM = pl.BlockSpec(memory_space=pltpu.SMEM)
HBM = pl.BlockSpec(memory_space=pl.ANY)
VMEM = pl.BlockSpec(memory_space=pltpu.VMEM)


def pack(send, near, lanes=None):
    rows, kmers = near[0].shape[1:]
    total = sum(ref.shape[0] for ref in near)
    lanes = lanes or [send.shape[0]]
    return pl.pallas_call(
        functools.partial(pack_kernel, len(lanes)),
        out_shape=[jax.ShapeDtypeStruct((lane, rows, kmers), near[0].dtype) for lane in lanes],
        in_specs=[SMEM] + [HBM] * len(near),
        out_specs=[VMEM] * len(lanes),
        scratch_shapes=[
            pltpu.VMEM((total, rows, kmers), near[0].dtype),
            pltpu.SemaphoreType.DMA((len(near),)),
        ],
        compiler_params=pltpu.CompilerParams(vmem_limit_bytes=60 << 20),
        name="pack",
    )(send, *near)


def tiles(pick, read_block, near):
    rows, kmers = near[0].shape[1:]
    total = sum(ref.shape[0] for ref in near) + 1
    return pl.pallas_call(
        tile_kernel,
        out_shape=jax.ShapeDtypeStruct((RB_DEV * rows, CAP * rows), jnp.float32),
        in_specs=[SMEM, SMEM] + [HBM] * len(near),
        out_specs=VMEM,
        scratch_shapes=[
            pltpu.VMEM((total, rows, kmers), near[0].dtype),
            pltpu.SemaphoreType.DMA((len(near),)),
        ],
        compiler_params=pltpu.CompilerParams(vmem_limit_bytes=60 << 20),
        name="tiles",
    )(pick, read_block, *near)


def greet(others):
    barrier = pltpu.get_barrier_semaphore()
    for other in others:
        pl.semaphore_signal(
            barrier, inc=1, device_id=(other,), device_id_type=pl.DeviceIdType.MESH
        )
    pl.semaphore_wait(barrier, len(others))


def everyone_kernel(
    devices, row_ref, mine_ref, owners_ref, orders_ref, sibling_ref, lead_ref, got, lead, *sems
):
    send_sems, recv_sems, move_sems = sems
    me = lax.axis_index("dev")
    load = pltpu.make_async_copy(mine_ref.at[pl.ds(0, lead.shape[0])], lead, move_sems.at[0])
    load.start()
    got[me] = row_ref[...]
    greet([(me + k) % devices for k in range(1, devices)])
    copies = [
        pltpu.make_async_remote_copy(
            src_ref=row_ref,
            dst_ref=got.at[me],
            send_sem=send_sems.at[k],
            recv_sem=recv_sems.at[k],
            device_id=((me + k) % devices,),
            device_id_type=pl.DeviceIdType.MESH,
        )
        for k in range(1, devices)
    ]
    for copy in copies:
        copy.start()
    swap = pltpu.make_async_remote_copy(
        src_ref=mine_ref,
        dst_ref=sibling_ref,
        send_sem=send_sems.at[0],
        recv_sem=recv_sems.at[0],
        device_id=(me + 1 - 2 * (me % CORES),),
        device_id_type=pl.DeviceIdType.MESH,
    )
    swap.start()
    load.wait()
    store = pltpu.make_async_copy(lead, lead_ref, move_sems.at[1])
    store.start()
    for copy in copies:
        copy.wait()
    owners_ref[...] = got[:, 0, :]
    orders_ref[...] = got[:, 1, :]
    store.wait()
    swap.wait()


def gather_rows(row, mine, kept):
    devices = lax.axis_size("dev")
    slots = row.shape[1]
    table = jax.ShapeDtypeStruct((devices, slots), row.dtype)
    lead = (kept,) + mine.shape[1:]
    return pl.pallas_call(
        functools.partial(everyone_kernel, devices),
        out_shape=[
            table,
            table,
            jax.ShapeDtypeStruct(mine.shape, mine.dtype),
            jax.ShapeDtypeStruct(lead, mine.dtype),
        ],
        in_specs=[VMEM, HBM],
        out_specs=[VMEM, VMEM, HBM, HBM],
        scratch_shapes=[
            pltpu.VMEM((devices,) + row.shape, row.dtype),
            pltpu.VMEM(lead, mine.dtype),
            pltpu.SemaphoreType.DMA((devices,)),
            pltpu.SemaphoreType.DMA((devices,)),
            pltpu.SemaphoreType.DMA((2,)),
        ],
        compiler_params=pltpu.CompilerParams(has_side_effects=True, collective_id=0),
        name="gather_rows",
    )(row, mine)


def flipped(value, mask):
    bit = 1
    while bit <= mask:
        if mask & bit:
            value = value + bit - 2 * bit * (value // bit % 2)
        bit *= 2
    return value


def exchange_kernel(devices, lane, out_ref, got_ref, send_sems, recv_sems):
    me = lax.axis_index("dev")
    count = devices // HALVES
    spot = me % count

    def copy_of(k):
        to = flipped(spot, k)
        return pltpu.make_async_remote_copy(
            src_ref=out_ref.at[pl.ds(to * lane, lane)],
            dst_ref=got_ref.at[pl.ds(spot * lane, lane)],
            send_sem=send_sems.at[k],
            recv_sem=recv_sems.at[k],
            device_id=(me - spot + to,),
            device_id_type=pl.DeviceIdType.MESH,
        )

    chips = count // CORES
    steps = []
    for mask in range(chips - 1, chips // 2 - 1, -1):
        for core in range(CORES):
            masks = [m for m in (mask, chips - 1 - mask) if m]
            steps.append([copy_of(m * CORES + core) for m in masks])
    for i, step in enumerate(steps):
        if i >= 2:
            for copy in steps[i - 2]:
                copy.wait_send()
        for copy in step:
            copy.start()
    for step in steps[-2:]:
        for copy in step:
            copy.wait_send()
    for step in steps:
        for copy in step:
            copy.wait_recv()


def exchange(out, lane):
    devices = lax.axis_size("dev")
    count = devices // HALVES
    return pl.pallas_call(
        functools.partial(exchange_kernel, devices, lane),
        out_shape=jax.ShapeDtypeStruct(out.shape, out.dtype),
        in_specs=[HBM],
        out_specs=HBM,
        scratch_shapes=[pltpu.SemaphoreType.DMA((count,))] * 2,
        compiler_params=pltpu.CompilerParams(has_side_effects=True),
        cost_estimate=pl.CostEstimate(
            flops=0, bytes_accessed=32 * out.size * out.dtype.itemsize, transcendentals=0
        ),
        name="exchange",
    )(out)


def trade_kernel(devices, early, late, cuts, *refs):
    send_ref, mine_ref, sibling_ref, far_ref, cross_ref = refs[:5]
    got_ref, also_ref, far_twin_ref, own_ref, twin_ref, held, crossed, first, lanes = refs[5:14]
    fill_sems, cross_sems, soon_sems, last_sems = refs[14:]
    families = devices // FAMILY
    me = lax.axis_index("dev")
    chip, core = me // CORES, me % CORES
    spot = chip % families
    twin, opposite = chip * CORES + 1 - core, (me + devices // HALVES) % devices
    blocks, kept, side = mine_ref.shape[0], far_ref.shape[0], cross_ref.shape[0]
    at = {"far": CORES * blocks, "far_twin": CORES * blocks + kept}

    def part(name, begin, size):
        if name in at:
            return held.at[pl.ds(at[name] + begin, size)]
        return crossed.at[pl.ds(begin if name == "own" else side + begin, size)]

    def remote(src, dst, send_sem, recv_sem, to):
        return pltpu.make_async_remote_copy(
            src_ref=src,
            dst_ref=dst,
            send_sem=send_sem,
            recv_sem=recv_sem,
            device_id=(to,),
            device_id_type=pl.DeviceIdType.MESH,
        )

    fills = [
        pltpu.make_async_copy(mine_ref, held.at[pl.ds(0, blocks)], fill_sems.at[0]),
        pltpu.make_async_copy(sibling_ref, held.at[pl.ds(blocks, blocks)], fill_sems.at[1]),
        pltpu.make_async_copy(far_ref, part("far", 0, kept), fill_sems.at[2]),
    ]
    for copy in fills:
        copy.start()
    chips = {k: (chip - spot + flipped(spot, k)) * CORES + core for k in range(1, families)}
    greet(list(chips.values()) + [twin, opposite])

    crossing, passing = [], []
    for i, (begin, size) in enumerate(cuts):
        here = part("own", begin, size)
        crossing.append(
            remote(
                cross_ref.at[pl.ds(begin, size)],
                here,
                cross_sems.at[4 * i],
                cross_sems.at[4 * i + 1],
                opposite,
            )
        )
        passing.append(
            remote(
                here,
                part("twin", begin, size),
                cross_sems.at[4 * i + 2],
                cross_sems.at[4 * i + 3],
                twin,
            )
        )
    last = 4 * len(cuts)
    share = remote(
        far_ref, part("far_twin", 0, kept), cross_sems.at[last], cross_sems.at[last + 1], twin
    )
    for copy in crossing:
        copy.start()
    share.start()

    top = families - 1
    steps = [[k for k in (m, top - m) if k] for m in range(top, families // 2 - 1, -1)]

    def lanes_of(src_ref, dst_ref, lane, sems):
        size = lane // CORES
        sent, passed = [], []
        for step in steps:
            sent.append([])
            passed.append([])
            for k in step:
                begin = k * lane + core * size
                rows = dst_ref.at[pl.ds(begin, size)]
                src = src_ref.at[pl.ds(k * size, size)]
                sent[-1].append(remote(src, rows, sems.at[4 * k], sems.at[4 * k + 1], chips[k]))
                passed[-1].append(
                    remote(rows, rows, sems.at[4 * k + 2], sems.at[4 * k + 3], twin)
                )
        return sent, passed

    def start(sent, i):
        for copy in sent[i]:
            copy.start()

    def finish(sent, i):
        for copy in sent[i]:
            copy.wait_send()

    def land(sent, passed, i):
        for copy, follow in zip(sent[i], passed[i]):
            copy.wait_recv()
            follow.start()

    base = held.shape[0]

    def block_of(at, everything):
        if not everything:
            return held[at]
        near = held[jnp.minimum(at, base - 1)]
        return jnp.where(at < base, near, crossed[jnp.maximum(at - base, 0)])

    def gather(into, skip, size, everything):
        for step in steps:
            for k in step:

                def move(i, _):
                    into[k * size + i] = block_of(send_ref[skip + k * size + i], everything)
                    return 0

                lax.fori_loop(0, size, move, 0, unroll=2)

    for copy in fills:
        copy.wait()
    share.wait_recv()
    gather(first, 0, early // CORES, False)
    count = len(steps)
    ahead, behind = (min(most, count) for most in AHEAD)
    soon, soon_passed = lanes_of(first, got_ref, early, soon_sems)
    for i in range(count):
        if i >= ahead:
            finish(soon, i - ahead)
        start(soon, i)
        if i >= ahead:
            land(soon, soon_passed, i - ahead)

    for copy, follow in zip(crossing, passing):
        copy.wait_recv()
        follow.start()
    for follow in passing:
        follow.wait_recv()
    stores = [
        pltpu.make_async_copy(part("far_twin", 0, kept), far_twin_ref, fill_sems.at[3]),
        pltpu.make_async_copy(part("own", 0, side), own_ref, fill_sems.at[4]),
        pltpu.make_async_copy(part("twin", 0, side), twin_ref, fill_sems.at[5]),
    ]
    for copy in stores:
        copy.start()

    gather(lanes, families * (early // CORES), late // CORES, True)
    late_sent, late_passed = lanes_of(lanes, also_ref, late, last_sems)
    for i in range(count + behind):
        if i >= behind:
            finish(late_sent, i - behind)
        if i < count:
            start(late_sent, i)
        if i == count - 1:
            for j in range(count - ahead, count):
                finish(soon, j)
                land(soon, soon_passed, j)
        if i >= behind:
            land(late_sent, late_passed, i - behind)
    for copy in crossing + passing + [share]:
        copy.wait_send()
    for copy in stores:
        copy.wait()
    for step in soon_passed + late_passed:
        for follow in step:
            follow.wait()


def trade(send, mine, sibling, far, crossing, early, late):
    devices = lax.axis_size("dev")
    families = devices // FAMILY
    shape, kind = mine.shape[1:], mine.dtype
    kept, side = far.shape[0], crossing.shape[0]
    cuts = [(0, side // 2), (side // 2, side - side // 2)]
    held = CORES * (mine.shape[0] + kept)

    def rows(count):
        return jax.ShapeDtypeStruct((count,) + shape, kind)

    return pl.pallas_call(
        functools.partial(trade_kernel, devices, early, late, cuts),
        out_shape=[
            rows(families * early),
            rows(families * late),
            rows(kept),
            rows(side),
            rows(side),
        ],
        in_specs=[SMEM] + [HBM] * 4,
        out_specs=[HBM] * 5,
        scratch_shapes=[
            pltpu.VMEM((held,) + shape, kind),
            pltpu.VMEM((CORES * side,) + shape, kind),
            pltpu.VMEM((families * early // CORES,) + shape, kind),
            pltpu.VMEM((families * late // CORES,) + shape, kind),
            pltpu.SemaphoreType.DMA((6,)),
            pltpu.SemaphoreType.DMA((4 * len(cuts) + 2,)),
            pltpu.SemaphoreType.DMA((4 * families,)),
            pltpu.SemaphoreType.DMA((4 * families,)),
        ],
        compiler_params=pltpu.CompilerParams(
            has_side_effects=True, collective_id=1, vmem_limit_bytes=60 << 20
        ),
        name="trade",
    )(send, mine, sibling, far, crossing)


def shards(occurrence, block_owner, read_block, slot_order):
    devices = lax.axis_size("dev")
    blocks = occurrence.shape[0]
    slots = slot_order.shape[1]
    spill = 2 * blocks // devices
    early, late, kept, cross = lane_sizes(blocks, devices)
    swap = [(d, d ^ 1) for d in range(devices)]
    across = [(d, (d + devices // HALVES) % devices) for d in range(devices)]
    row = jnp.stack([jnp.pad(block_owner[:, 0], (0, slots - blocks)), slot_order[0]])
    mine = occurrence
    owners, orders, sibling, lead = gather_rows(row, mine, kept)
    far = lax.ppermute(lead, "dev", across)
    table = group_table(owners[:, :blocks], orders)
    sizes = blocks, early, late, kept, cross
    cross_send, known = plan(table, *sizes)
    crossing = pack(cross_send, (mine, sibling))[0]
    send, pick = late_plan(known, *sizes)
    full = too_full(table, *sizes)
    far, send, pick, full = lax.optimization_barrier((far, send, pick, full))
    got, also, far_twin, own, twin = trade(send, mine, sibling, far, crossing, early, late)
    first = tiles(pick, read_block, (mine, sibling, far, far_twin, own, twin, got, also))

    def more(carry):
        begin, _, margin = carry
        begin, now, mine = lax.optimization_barrier((begin, table, occurrence))
        send, pick, local = routes(now, blocks)
        sibling = lax.ppermute(mine, "dev", swap)
        far = lax.ppermute(mine, "dev", across)
        near = (mine, sibling, far, lax.ppermute(far, "dev", swap))
        got = exchange(pack(send(begin, spill, False), near[:CORES])[0], spill)
        also = exchange(pack(send(begin, spill, True), near[CORES:])[0], spill)
        added = tiles(pick(begin, spill, local), read_block, near + (got, also))
        margin = jnp.where(begin == 0, 0.0, margin) + added
        return begin + CORES * spill, i32(fullest_lane(now, blocks)), margin

    start = jnp.int32(0), jnp.where(full, 1, 0).astype(jnp.int32), first
    return lax.while_loop(lambda carry: carry[0] < carry[1], more, start)[2]


def solution(mesh):
    placed = (P("dev", None, None), P("dev", None), P("dev"), P("dev", None))
    return jax.shard_map(
        shards, mesh=mesh, in_specs=placed, out_specs=P("dev", None), check_vma=False
    )
```

```python
import functools
import jax
import jax.numpy as jnp
import numpy as np
from jax import lax
from jax.experimental import pallas as pl
from jax.experimental.pallas import tpu as pltpu
from jax.sharding import PartitionSpec as P

CAP = 4
RB_DEV = 16
CORES = 2
HALVES = 2
FAMILY = CORES * HALVES
AHEAD = 4, 4
TOGETHER = 4


def i32(x):
    return x.astype(jnp.int32)


def iota(*shape, axis):
    return lax.broadcasted_iota(jnp.int32, shape, axis)


def group_table(owners, order):
    devices, blocks = owners.shape
    slots = order.shape[1]
    per_pair = slots // devices
    earlier = iota(blocks, blocks, axis=1) < iota(blocks, blocks, axis=0)
    same = owners[:, :, None] == owners[:, None, :]
    rank = jnp.sum(i32(same & earlier[None]), axis=2)
    key = owners * per_pair + rank
    number = iota(devices, blocks, axis=0) * blocks + iota(devices, blocks, axis=1) + 1
    hit = key[:, :, None] == iota(1, 1, slots, axis=2)
    holder = jnp.sum(jnp.where(hit, number[:, :, None], 0), axis=1)
    holder = holder.reshape(devices, devices, per_pair).transpose(1, 0, 2).reshape(devices, slots)
    turned = order.reshape(devices, slots // CAP, CAP).transpose(2, 0, 1)
    hit = turned[:, :, :, None] == iota(1, 1, 1, slots, axis=3)
    table = jnp.sum(jnp.where(hit, holder[None, :, None, :], 0), axis=3)
    return table.reshape(CAP, devices * slots // CAP)


def fullest_lane(table, blocks):
    devices = lax.axis_size("dev")
    families = devices // FAMILY
    chips = devices // CORES
    source = jnp.where(table > 0, (table - 1) // blocks, -1)
    named = source[:, :, None] == iota(1, 1, devices, axis=2)
    held = jnp.sum(i32(named), axis=0)
    held_chip = jnp.sum(held.reshape(-1, chips, CORES), axis=2)
    demand = jnp.einsum(
        "gc,gd->cd",
        held_chip.astype(jnp.bfloat16),
        (held > 0).astype(jnp.bfloat16),
        preferred_element_type=jnp.float32,
    )
    c, d = iota(chips, devices, axis=0), iota(chips, devices, axis=1)
    return jnp.max(jnp.where(c % families != d // CORES % families, demand, 0.0))


def routes(table, blocks):
    devices = lax.axis_size("dev")
    families = devices // FAMILY
    half_devices = devices // HALVES
    many = FAMILY * blocks
    me = lax.axis_index("dev")
    half, family, core = me // half_devices, me // CORES % families, me % CORES
    x = jnp.arange(many, dtype=jnp.int32)
    x_half, x_core, x_block = x // (CORES * blocks), x // blocks % CORES, x % blocks
    ids = (((x_half * families + family) * CORES + x_core) * blocks + x_block + 1)[:, None]
    inside = (table[0][None] == ids) | (table[1][None] == ids)
    for j in range(2, CAP):
        inside = inside | (table[j][None] == ids)
    partners = jnp.stack(
        [jnp.sum(jnp.where(inside, table[j][None], 0), axis=1) for j in range(CAP)]
    )
    source = jnp.where(partners > 0, (partners - 1) // blocks, -1)
    target = iota(1, half_devices, axis=1) + half * half_devices
    named = source[:, :, None] == target[None]
    need = jnp.any(named, axis=0) & (target // CORES % families != family)
    row, column = iota(many, many, axis=0), iota(many, many, axis=1)
    same_chip = row // (CORES * blocks) == column // (CORES * blocks)
    before = ((column < row) & same_chip).astype(jnp.bfloat16)
    rank = i32(jnp.dot(before, need.astype(jnp.bfloat16), preferred_element_type=jnp.float32))
    rank = jnp.where(need, rank, -1).T
    local = (i32(x_half != half) * CORES + i32(x_core != core)) * blocks + x_block

    begin = half * CORES * blocks + core * blocks
    own = lax.dynamic_slice(partners, (0, begin), (CAP, blocks)).reshape(-1)
    total = devices * blocks
    match = own[:, None] == iota(1, total, axis=1) + 1
    wanted = jnp.any(match, axis=0).reshape(HALVES, families, CORES * blocks)
    wanted = wanted.transpose(1, 0, 2).reshape(families, many)
    arrived = i32(
        jnp.dot(wanted.astype(jnp.bfloat16), before.T, preferred_element_type=jnp.float32)
    )
    f = iota(families, many, axis=0)
    part = i32(iota(families, many, axis=1) // (CORES * blocks) != half)

    def send(begin, lane, far):
        spot = begin + iota(1, lane, 1, axis=1) * CORES + core
        chosen = jnp.where((x_half != half) == far, local % (CORES * blocks), 0)
        hit = (rank[:, None, :] == spot) & ((x_half != half) == far)
        return jnp.sum(jnp.where(hit, chosen[None, None, :], 0), axis=2).reshape(-1)

    def pick(begin, lane, local):
        empty = many + HALVES * half_devices * lane
        now = arrived - begin
        there = (part * half_devices + f * CORES + now % CORES) * lane + now // CORES + many
        there = jnp.where((now >= 0) & (now < lane * CORES), there, empty)
        place = jnp.where((f == family) & (begin == 0), local[None, :], jnp.where(f == family, empty, there))
        place = place.reshape(families, HALVES, CORES * blocks).transpose(1, 0, 2).reshape(1, total)
        found = jnp.sum(jnp.where(match, place, 0), axis=1)
        return jnp.where(own > 0, found, empty)

    return send, pick, local


def lane_sizes(blocks, devices):
    share = max(1, CORES * blocks * CORES // devices)
    soon, rest = 2.1 * share, 1.26 * share
    early = CORES * round((soon + 0.8 * soon**0.5) / CORES)
    late = CORES * round((rest + 4.4 * rest**0.5) / CORES)
    kept = blocks // 4
    cross = 37 * (CORES * (blocks - kept)) // 48
    return early, late, kept, cross - cross % CORES


def chip_counts(table, blocks, kept):
    devices = lax.axis_size("dev")
    chips = devices // CORES
    source = jnp.where(table > 0, (table - 1) // (blocks * CORES), -1)
    spot = (table - 1) % blocks
    named = source[:, :, None] == iota(1, 1, chips, axis=2)
    held = jnp.sum(i32(named), axis=0)
    packed = jnp.sum(i32(named & (spot >= kept)[:, :, None]), axis=0)
    return held, packed


def too_full(table, blocks, early, late, kept, cross):
    devices = lax.axis_size("dev")
    chips = devices // CORES
    families = devices // FAMILY
    held, packed = chip_counts(table, blocks, kept)
    here = (held > 0).astype(jnp.bfloat16)
    both = jnp.concatenate([held, packed], axis=1).astype(jnp.bfloat16)
    demand = jnp.einsum("gc,gd->cd", both, here, preferred_element_type=jnp.float32)
    demand, last = demand[:chips], demand[chips:]
    c, d = iota(chips, chips, axis=0), iota(chips, chips, axis=1)
    beyond = c // families != d // families

    def turned(far):
        return jnp.concatenate([far[families:], far[:families]], axis=0)

    last = turned(jnp.where(beyond, last, 0.0))
    soon = jnp.where(beyond, 0.0, demand) + turned(jnp.where(beyond, demand, 0.0)) - last
    load = last + jnp.maximum(soon - early, 0.0)
    load = jnp.max(jnp.where(c % families != d % families, load, 0.0))
    halves = jnp.max(here.reshape(-1, HALVES, families), axis=2)
    crossing = jnp.einsum(
        "gc,gh->ch", packed.astype(jnp.bfloat16), halves, preferred_element_type=jnp.float32
    )
    c, h = iota(chips, HALVES, axis=0), iota(chips, HALVES, axis=1)
    crossing = jnp.max(jnp.where(c // families != h, crossing, 0.0))
    return (load > late) | (crossing > cross)


def orders_of(blocks, kept):
    devices = lax.axis_size("dev")
    families = devices // FAMILY
    me = lax.axis_index("dev")
    half, family, core = me // (devices // HALVES), me // CORES % families, me % CORES
    part = np.repeat(np.arange(HALVES), CORES * blocks)
    x_core = np.tile(np.repeat(np.arange(CORES), blocks), HALVES)
    x_block = np.tile(np.arange(blocks), FAMILY)
    order = np.lexsort((x_block, x_core, (part == 1) & (x_block >= kept), part))
    part, x_core, x_block = (jnp.asarray(v[order], jnp.int32) for v in (part, x_core, x_block))
    return half, family, core, part, x_core, x_block


def plan(table, blocks, early, late, kept, cross):
    devices = lax.axis_size("dev")
    families = devices // FAMILY
    many = FAMILY * blocks
    pair = CORES * blocks
    half, family, core, part, x_core, x_block = orders_of(blocks, kept)
    x_half = jnp.where(half == 0, part, 1 - part)
    away = jnp.where(core == 0, x_core, 1 - x_core)

    ids = (((x_half * families + family) * CORES + x_core) * blocks + x_block + 1)[:, None]
    inside = (table[0][None] == ids) | (table[1][None] == ids)
    for j in range(2, CAP):
        inside = inside | (table[j][None] == ids)
    partners = jnp.stack(
        [jnp.sum(jnp.where(inside, table[j][None], 0), axis=1) for j in range(CAP)]
    )
    chip = jnp.where(partners > 0, (partners - 1) // pair, -1)
    mask = iota(1, families, axis=1)
    target = (family ^ mask) + half * families
    need = jnp.any(chip[:, :, None] == target[None], axis=0) & (mask > 0)
    crosses = jnp.any((partners > 0) & (chip // families != x_half[None]), axis=0)
    crosses = crosses & (x_block >= kept)
    leaves, comes = crosses & (part == 0), crosses & (part == 1)
    wide = jnp.concatenate([need, leaves[:, None], comes[:, None]], axis=1)
    before = (iota(many, many, axis=1) < iota(many, many, axis=0)).astype(jnp.bfloat16)
    ranks = i32(jnp.dot(before, wide.astype(jnp.bfloat16), preferred_element_type=jnp.float32))
    ranks = jnp.where(wide, ranks, -1).T
    rank, leaving, coming = ranks[:families], ranks[families], ranks[families + 1]
    side = cross // CORES
    second = i32(coming >= side)
    packed = pair + CORES * kept
    packed = packed + jnp.where(core == 0, second, 1 - second) * side + coming - second * side
    local = jnp.where(
        part == 0,
        away * blocks + x_block,
        jnp.where(x_block < kept, pair + away * kept + x_block, packed),
    )

    spots = iota(1, side, 1, axis=1)[0] + core * side
    cross_send = jnp.sum(jnp.where(leaving[None] == spots, local[None], 0), axis=1)

    return cross_send, (partners, rank, need, local)


def late_plan(known, blocks, early, late, kept, cross):
    partners, rank, need, local = known
    devices = lax.axis_size("dev")
    families = devices // FAMILY
    many = FAMILY * blocks
    pair = CORES * blocks
    half, family, core, part, x_core, x_block = orders_of(blocks, kept)
    x_half = jnp.where(half == 0, part, 1 - part)
    soon = (part == 0) | (x_block < kept)
    shipped = jnp.minimum(jnp.sum(i32(need & soon[:, None]), axis=0), early)

    def send(first, allowed, side):
        spot = first[:, None, None] + iota(1, side, 1, axis=1) + core * side
        hit = (rank[:, None, :] == spot) & allowed
        return jnp.sum(jnp.where(hit, local[None, None, :], 0), axis=2).reshape(-1)

    sends = send(0 * shipped, soon[None, None, :], early // CORES), send(shipped, True, late // CORES)
    mask = iota(families, 1, axis=0)
    pairs = partners[:, :pair].reshape(-1)
    all_ids = (
        ((x_half[None] * families + (family ^ mask)) * CORES + x_core[None]) * blocks
        + x_block[None]
        + 1
    ).reshape(1, -1)
    wanted = jnp.any(pairs[:, None] == all_ids, axis=0).reshape(families, many)
    before = (iota(many, many, axis=0) < iota(many, many, axis=1)).astype(jnp.bfloat16)
    arrived = i32(
        jnp.dot(wanted.astype(jnp.bfloat16), before, preferred_element_type=jnp.float32)
    )
    came = jnp.sum(i32(wanted & soon[None]), axis=1, keepdims=True)
    came = jnp.minimum(came, early)
    base = pair + CORES * kept + cross
    place = jnp.where(
        arrived < came,
        base + mask * early + arrived,
        base + families * early + mask * late + arrived - came,
    )
    place = jnp.where(mask == 0, local[None], place).reshape(1, -1)
    empty = base + families * (early + late)
    own = lax.dynamic_slice(partners, (0, core * blocks), (CAP, blocks)).reshape(-1)
    picked = jnp.sum(jnp.where(own[:, None] == all_ids, place, 0), axis=1)
    pick = jnp.where(own > 0, picked, empty)
    waits = (pick >= base + families * early) & (pick < empty)
    waits = jnp.any(waits.reshape(CAP, blocks), axis=0)
    return jnp.concatenate(sends), pick, waits


def turn_of(waits):
    blocks = waits.shape[0]
    number = iota(blocks, blocks, axis=1)
    key = i32(waits) * blocks + number[0]
    spot = jnp.sum(i32(key[None, :] < key[:, None]), axis=1)
    turn = jnp.sum(jnp.where(spot[:, None] == iota(1, blocks, axis=1), number.T, 0), axis=0)
    return jnp.concatenate([turn, jnp.sum(i32(~waits))[None]])


def fill(refs, held, sems):
    copies, at = [], 0
    for i, ref in enumerate(refs):
        copies.append(
            pltpu.make_async_copy(ref, held.at[pl.ds(at, ref.shape[0])], sems.at[i])
        )
        copies[-1].start()
        at += ref.shape[0]
    return copies


def pack_kernel(parts, send_ref, *refs):
    near, outs, (held, sems) = refs[: -2 - parts], refs[-2 - parts : -2], refs[-2:]
    for copy in fill(near, held, sems):
        copy.wait()
    begin = 0
    for out_ref in outs:

        def step(i, _):
            out_ref[i] = held[send_ref[begin + i]]
            return 0

        lax.fori_loop(0, out_ref.shape[0], step, 0, unroll=2)
        begin += out_ref.shape[0]


def tile_kernel(pick_ref, read_ref, turn_ref, *refs):
    near, (out_ref, held, sems) = refs[:-3], refs[-3:]
    blocks, rows = near[0].shape[:2]
    copies = fill(near, held, sems)
    held[held.shape[0] - 1] = jnp.zeros(held.shape[1:], held.dtype)
    out_ref[...] = jnp.zeros_like(out_ref)
    for copy in copies[:-1]:
        copy.wait()

    def tile_of(b):
        others = jnp.concatenate([held[pick_ref[j * blocks + b]] for j in range(CAP)], axis=0)
        tile = lax.dot_general(
            held[b], others, (((1,), (1,)), ((), ())), preferred_element_type=jnp.float32
        )
        return tile.astype(jnp.bfloat16)

    def step(i, _):
        now = [turn_ref[i * TOGETHER + k] for k in range(TOGETHER)]
        found = [tile_of(b) for b in now]
        for k in range(TOGETHER):
            begin = read_ref[now[k]] * rows
            where = pl.ds(pl.multiple_of(begin, rows), rows)
            out_ref[where, :] += found[k].astype(jnp.float32)
        return 0

    def two(i, _):
        return step(2 * i + 1, step(2 * i, 0))

    ready = turn_ref[blocks] // (2 * TOGETHER)
    lax.fori_loop(0, ready, two, 0)
    copies[-1].wait()
    lax.fori_loop(ready, blocks // (2 * TOGETHER), two, 0)


SMEM = pl.BlockSpec(memory_space=pltpu.SMEM)
HBM = pl.BlockSpec(memory_space=pl.ANY)
VMEM = pl.BlockSpec(memory_space=pltpu.VMEM)


def pack(send, near, lanes=None):
    rows, kmers = near[0].shape[1:]
    total = sum(ref.shape[0] for ref in near)
    lanes = lanes or [send.shape[0]]
    return pl.pallas_call(
        functools.partial(pack_kernel, len(lanes)),
        out_shape=[jax.ShapeDtypeStruct((lane, rows, kmers), near[0].dtype) for lane in lanes],
        in_specs=[SMEM] + [HBM] * len(near),
        out_specs=[VMEM] * len(lanes),
        scratch_shapes=[
            pltpu.VMEM((total, rows, kmers), near[0].dtype),
            pltpu.SemaphoreType.DMA((len(near),)),
        ],
        compiler_params=pltpu.CompilerParams(vmem_limit_bytes=60 << 20),
        name="pack",
    )(send, *near)


def tiles(pick, read_block, turn, near):
    rows, kmers = near[0].shape[1:]
    total = sum(ref.shape[0] for ref in near) + 1
    return pl.pallas_call(
        tile_kernel,
        out_shape=jax.ShapeDtypeStruct((RB_DEV * rows, CAP * rows), jnp.float32),
        in_specs=[SMEM, SMEM, SMEM] + [HBM] * len(near),
        out_specs=VMEM,
        scratch_shapes=[
            pltpu.VMEM((total, rows, kmers), near[0].dtype),
            pltpu.SemaphoreType.DMA((len(near),)),
        ],
        compiler_params=pltpu.CompilerParams(vmem_limit_bytes=60 << 20),
        name="tiles",
    )(pick, read_block, turn, *near)


def greet(others):
    barrier = pltpu.get_barrier_semaphore()
    for other in others:
        pl.semaphore_signal(
            barrier, inc=1, device_id=(other,), device_id_type=pl.DeviceIdType.MESH
        )
    pl.semaphore_wait(barrier, len(others))


def everyone_kernel(
    devices, row_ref, mine_ref, owners_ref, orders_ref, sibling_ref, lead_ref, got, lead, *sems
):
    send_sems, recv_sems, move_sems = sems
    me = lax.axis_index("dev")
    load = pltpu.make_async_copy(mine_ref.at[pl.ds(0, lead.shape[0])], lead, move_sems.at[0])
    load.start()
    got[me] = row_ref[...]
    greet([(me + k) % devices for k in range(1, devices)])
    copies = [
        pltpu.make_async_remote_copy(
            src_ref=row_ref,
            dst_ref=got.at[me],
            send_sem=send_sems.at[k],
            recv_sem=recv_sems.at[k],
            device_id=((me + k) % devices,),
            device_id_type=pl.DeviceIdType.MESH,
        )
        for k in range(1, devices)
    ]
    for copy in copies:
        copy.start()
    swap = pltpu.make_async_remote_copy(
        src_ref=mine_ref,
        dst_ref=sibling_ref,
        send_sem=send_sems.at[0],
        recv_sem=recv_sems.at[0],
        device_id=(me + 1 - 2 * (me % CORES),),
        device_id_type=pl.DeviceIdType.MESH,
    )
    swap.start()
    load.wait()
    store = pltpu.make_async_copy(lead, lead_ref, move_sems.at[1])
    store.start()
    for copy in copies:
        copy.wait()
    owners_ref[...] = got[:, 0, :]
    orders_ref[...] = got[:, 1, :]
    store.wait()
    swap.wait()


def gather_rows(row, mine, kept):
    devices = lax.axis_size("dev")
    slots = row.shape[1]
    table = jax.ShapeDtypeStruct((devices, slots), row.dtype)
    lead = (kept,) + mine.shape[1:]
    return pl.pallas_call(
        functools.partial(everyone_kernel, devices),
        out_shape=[
            table,
            table,
            jax.ShapeDtypeStruct(mine.shape, mine.dtype),
            jax.ShapeDtypeStruct(lead, mine.dtype),
        ],
        in_specs=[VMEM, HBM],
        out_specs=[VMEM, VMEM, HBM, HBM],
        scratch_shapes=[
            pltpu.VMEM((devices,) + row.shape, row.dtype),
            pltpu.VMEM(lead, mine.dtype),
            pltpu.SemaphoreType.DMA((devices,)),
            pltpu.SemaphoreType.DMA((devices,)),
            pltpu.SemaphoreType.DMA((2,)),
        ],
        compiler_params=pltpu.CompilerParams(has_side_effects=True, collective_id=0),
        name="gather_rows",
    )(row, mine)


def flipped(value, mask):
    bit = 1
    while bit <= mask:
        if mask & bit:
            value = value + bit - 2 * bit * (value // bit % 2)
        bit *= 2
    return value


def exchange_kernel(devices, lane, out_ref, got_ref, send_sems, recv_sems):
    me = lax.axis_index("dev")
    count = devices // HALVES
    spot = me % count

    def copy_of(k):
        to = flipped(spot, k)
        return pltpu.make_async_remote_copy(
            src_ref=out_ref.at[pl.ds(to * lane, lane)],
            dst_ref=got_ref.at[pl.ds(spot * lane, lane)],
            send_sem=send_sems.at[k],
            recv_sem=recv_sems.at[k],
            device_id=(me - spot + to,),
            device_id_type=pl.DeviceIdType.MESH,
        )

    chips = count // CORES
    steps = []
    for mask in range(chips - 1, chips // 2 - 1, -1):
        for core in range(CORES):
            masks = [m for m in (mask, chips - 1 - mask) if m]
            steps.append([copy_of(m * CORES + core) for m in masks])
    for i, step in enumerate(steps):
        if i >= 2:
            for copy in steps[i - 2]:
                copy.wait_send()
        for copy in step:
            copy.start()
    for step in steps[-2:]:
        for copy in step:
            copy.wait_send()
    for step in steps:
        for copy in step:
            copy.wait_recv()


def exchange(out, lane):
    devices = lax.axis_size("dev")
    count = devices // HALVES
    return pl.pallas_call(
        functools.partial(exchange_kernel, devices, lane),
        out_shape=jax.ShapeDtypeStruct(out.shape, out.dtype),
        in_specs=[HBM],
        out_specs=HBM,
        scratch_shapes=[pltpu.SemaphoreType.DMA((count,))] * 2,
        compiler_params=pltpu.CompilerParams(has_side_effects=True),
        cost_estimate=pl.CostEstimate(
            flops=0, bytes_accessed=32 * out.size * out.dtype.itemsize, transcendentals=0
        ),
        name="exchange",
    )(out)


def trade_kernel(devices, early, late, cuts, *refs):
    send_ref, mine_ref, sibling_ref, far_ref, cross_ref = refs[:5]
    got_ref, also_ref, far_twin_ref, own_ref, twin_ref, held, crossed, first, lanes = refs[5:14]
    fill_sems, cross_sems, soon_sems, last_sems = refs[14:]
    families = devices // FAMILY
    me = lax.axis_index("dev")
    chip, core = me // CORES, me % CORES
    spot = chip % families
    twin, opposite = chip * CORES + 1 - core, (me + devices // HALVES) % devices
    blocks, kept, side = mine_ref.shape[0], far_ref.shape[0], cross_ref.shape[0]
    at = {"far": CORES * blocks, "far_twin": CORES * blocks + kept}

    def part(name, begin, size):
        if name in at:
            return held.at[pl.ds(at[name] + begin, size)]
        return crossed.at[pl.ds(begin if name == "own" else side + begin, size)]

    def remote(src, dst, send_sem, recv_sem, to):
        return pltpu.make_async_remote_copy(
            src_ref=src,
            dst_ref=dst,
            send_sem=send_sem,
            recv_sem=recv_sem,
            device_id=(to,),
            device_id_type=pl.DeviceIdType.MESH,
        )

    fills = [
        pltpu.make_async_copy(mine_ref, held.at[pl.ds(0, blocks)], fill_sems.at[0]),
        pltpu.make_async_copy(sibling_ref, held.at[pl.ds(blocks, blocks)], fill_sems.at[1]),
        pltpu.make_async_copy(far_ref, part("far", 0, kept), fill_sems.at[2]),
    ]
    for copy in fills:
        copy.start()
    chips = {k: (chip - spot + flipped(spot, k)) * CORES + core for k in range(1, families)}
    greet(list(chips.values()) + [twin, opposite])

    crossing, passing = [], []
    for i, (begin, size) in enumerate(cuts):
        here = part("own", begin, size)
        crossing.append(
            remote(
                cross_ref.at[pl.ds(begin, size)],
                here,
                cross_sems.at[4 * i],
                cross_sems.at[4 * i + 1],
                opposite,
            )
        )
        passing.append(
            remote(
                here,
                part("twin", begin, size),
                cross_sems.at[4 * i + 2],
                cross_sems.at[4 * i + 3],
                twin,
            )
        )
    last = 4 * len(cuts)
    share = remote(
        far_ref, part("far_twin", 0, kept), cross_sems.at[last], cross_sems.at[last + 1], twin
    )
    for copy in crossing:
        copy.start()
    share.start()

    top = families - 1
    steps = [[k for k in (m, top - m) if k] for m in range(top, families // 2 - 1, -1)]

    def lanes_of(src_ref, dst_ref, lane, sems):
        size = lane // CORES
        sent, passed = [], []
        for step in steps:
            sent.append([])
            passed.append([])
            for k in step:
                begin = k * lane + core * size
                rows = dst_ref.at[pl.ds(begin, size)]
                src = src_ref.at[pl.ds(k * size, size)]
                sent[-1].append(remote(src, rows, sems.at[4 * k], sems.at[4 * k + 1], chips[k]))
                passed[-1].append(
                    remote(rows, rows, sems.at[4 * k + 2], sems.at[4 * k + 3], twin)
                )
        return sent, passed

    def start(sent, i):
        for copy in sent[i]:
            copy.start()

    def finish(sent, i):
        for copy in sent[i]:
            copy.wait_send()

    def land(sent, passed, i):
        for copy, follow in zip(sent[i], passed[i]):
            copy.wait_recv()
            follow.start()

    base = held.shape[0]

    def block_of(at, everything):
        if not everything:
            return held[at]
        near = held[jnp.minimum(at, base - 1)]
        return jnp.where(at < base, near, crossed[jnp.maximum(at - base, 0)])

    def gather(into, skip, size, everything):
        for step in steps:
            for k in step:

                def move(i, _):
                    into[k * size + i] = block_of(send_ref[skip + k * size + i], everything)
                    return 0

                lax.fori_loop(0, size, move, 0, unroll=2)

    for copy in fills:
        copy.wait()
    share.wait_recv()
    gather(first, 0, early // CORES, False)
    count = len(steps)
    ahead, behind = (min(most, count) for most in AHEAD)
    soon, soon_passed = lanes_of(first, got_ref, early, soon_sems)
    for i in range(count):
        if i >= ahead:
            finish(soon, i - ahead)
        start(soon, i)
        if i >= ahead:
            land(soon, soon_passed, i - ahead)

    for copy, follow in zip(crossing, passing):
        copy.wait_recv()
        follow.start()
    for follow in passing:
        follow.wait_recv()
    stores = [
        pltpu.make_async_copy(part("far_twin", 0, kept), far_twin_ref, fill_sems.at[3]),
        pltpu.make_async_copy(part("own", 0, side), own_ref, fill_sems.at[4]),
        pltpu.make_async_copy(part("twin", 0, side), twin_ref, fill_sems.at[5]),
    ]
    for copy in stores:
        copy.start()

    gather(lanes, families * (early // CORES), late // CORES, True)
    late_sent, late_passed = lanes_of(lanes, also_ref, late, last_sems)
    for i in range(count + behind):
        if i >= behind:
            finish(late_sent, i - behind)
        if i < count:
            start(late_sent, i)
        if i == count - 1:
            for j in range(count - ahead, count):
                finish(soon, j)
                land(soon, soon_passed, j)
        if i >= behind:
            land(late_sent, late_passed, i - behind)
    for copy in crossing + passing + [share]:
        copy.wait_send()
    for copy in stores:
        copy.wait()
    for step in soon_passed + late_passed:
        for follow in step:
            follow.wait()


def trade(send, mine, sibling, far, crossing, early, late):
    devices = lax.axis_size("dev")
    families = devices // FAMILY
    shape, kind = mine.shape[1:], mine.dtype
    kept, side = far.shape[0], crossing.shape[0]
    most = 3 * side // 4
    cuts = [(0, most), (most, side - most)]
    held = CORES * (mine.shape[0] + kept)

    def rows(count):
        return jax.ShapeDtypeStruct((count,) + shape, kind)

    return pl.pallas_call(
        functools.partial(trade_kernel, devices, early, late, cuts),
        out_shape=[
            rows(families * early),
            rows(families * late),
            rows(kept),
            rows(side),
            rows(side),
        ],
        in_specs=[SMEM] + [HBM] * 4,
        out_specs=[HBM] * 5,
        scratch_shapes=[
            pltpu.VMEM((held,) + shape, kind),
            pltpu.VMEM((CORES * side,) + shape, kind),
            pltpu.VMEM((families * early // CORES,) + shape, kind),
            pltpu.VMEM((families * late // CORES,) + shape, kind),
            pltpu.SemaphoreType.DMA((6,)),
            pltpu.SemaphoreType.DMA((4 * len(cuts) + 2,)),
            pltpu.SemaphoreType.DMA((4 * families,)),
            pltpu.SemaphoreType.DMA((4 * families,)),
        ],
        compiler_params=pltpu.CompilerParams(
            has_side_effects=True, collective_id=1, vmem_limit_bytes=60 << 20
        ),
        name="trade",
    )(send, mine, sibling, far, crossing)


def shards(occurrence, block_owner, read_block, slot_order):
    devices = lax.axis_size("dev")
    blocks = occurrence.shape[0]
    slots = slot_order.shape[1]
    spill = 2 * blocks // devices
    early, late, kept, cross = lane_sizes(blocks, devices)
    swap = [(d, d ^ 1) for d in range(devices)]
    across = [(d, (d + devices // HALVES) % devices) for d in range(devices)]
    row = jnp.stack([jnp.pad(block_owner[:, 0], (0, slots - blocks)), slot_order[0]])
    mine = occurrence
    owners, orders, sibling, lead = gather_rows(row, mine, kept)
    far = lax.ppermute(lead, "dev", across)
    table = group_table(owners[:, :blocks], orders)
    sizes = blocks, early, late, kept, cross
    cross_send, known = plan(table, *sizes)
    crossing = pack(cross_send, (mine, sibling))[0]
    send, pick, waits = late_plan(known, *sizes)
    turn = turn_of(waits)
    full = too_full(table, *sizes)
    far, send, pick, turn, full = lax.optimization_barrier((far, send, pick, turn, full))
    got, also, far_twin, own, twin = trade(send, mine, sibling, far, crossing, early, late)
    first = tiles(pick, read_block, turn, (mine, sibling, far, far_twin, own, twin, got, also))

    def more(carry):
        begin, _, margin = carry
        begin, now, mine = lax.optimization_barrier((begin, table, occurrence))
        send, pick, local = routes(now, blocks)
        sibling = lax.ppermute(mine, "dev", swap)
        far = lax.ppermute(mine, "dev", across)
        near = (mine, sibling, far, lax.ppermute(far, "dev", swap))
        got = exchange(pack(send(begin, spill, False), near[:CORES])[0], spill)
        also = exchange(pack(send(begin, spill, True), near[CORES:])[0], spill)
        plain = turn_of(jnp.ones((blocks,), bool))
        added = tiles(pick(begin, spill, local), read_block, plain, near + (got, also))
        margin = jnp.where(begin == 0, 0.0, margin) + added
        return begin + CORES * spill, i32(fullest_lane(now, blocks)), margin

    start = jnp.int32(0), jnp.where(full, 1, 0).astype(jnp.int32), first
    return lax.while_loop(lambda carry: carry[0] < carry[1], more, start)[2]


def solution(mesh):
    placed = (P("dev", None, None), P("dev", None), P("dev"), P("dev", None))
    return jax.shard_map(
        shards, mesh=mesh, in_specs=placed, out_specs=P("dev", None), check_vma=False
    )
```
